32 devices in a mesh: shard: 32 (over z, y, x, core).
Axes of the slice: x: 2, y: 2, z: 4, core: 2. Of those that a mesh axis runs over, the one named last changes fastest.
Arguments:
- data_t: bfloat16 [8192, 8192], P('shard'), may hold values from -0.125 to 0.125
- labels: int32 [8192], replicated, may hold values from -1 to 1, as said below
- sample_weight: float32 [8192], replicated, may hold values from 0.1 to 4
- w_start: float32 [8192], P('shard'), may hold values from -10 to 10
- alpha_start: float32 [8192], P('shard'), may hold values from 0 to 1
- visit_order: int32 [64, 128], P('shard'), may hold values from 0 to 127, each once within a row
Outputs:
- weights_out: float32 [8192], P('shard')
- alpha_final: float32 [8192], P('shard')
- objective: float32 [], replicated
The draws below stay inside these ranges and needn't reach their ends.
Inputs may be any that keep to these rules, and one draw needn't show every extreme that they name: `labels`: each label is -1 or +1. `visit_order`: each row is a permutation of 0 to 127.
All inputs are finite; a program needn't handle non-finite values.
Results may differ from the reference program's by a relative error of at most 0.0047.
Values may be sent and summed in bfloat16 or wider, within the bound.
A program may use at most 64 MiB of HBM per device.

```python
import jax
import jax.numpy as jnp
from jax import lax

FEATURES = 8192
BLOCK = 128
GROUP = 16
SAMPLES = 8192
BLOCKS = 64
N_SHARD = 32


def draw_labels(key, part):
    return (2 * jax.random.randint(key, (SAMPLES,), 0, 2) - 1).astype(jnp.int32)


def draw_sample_weight(key, part):
    position = jnp.arange(SAMPLES, dtype=jnp.float32) / (SAMPLES - 1)
    roughness = jnp.exp(jax.random.uniform(key, (SAMPLES,), jnp.float32, -0.35, 0.35))
    return (0.5 * jnp.power(3.0, position) * roughness).astype(jnp.float32)


def draw_w_start(key, part):
    position = jnp.arange(FEATURES, dtype=jnp.float32) / (FEATURES - 1)
    normal_draw = jnp.clip(jax.random.normal(key, (FEATURES,), jnp.float32), -4.0, 4.0)
    return (0.6 * jnp.power(3.0, position) * normal_draw).astype(jnp.float32)


def with_spikes(array, stream_key, source, target, parts, factor):
    owner, partner = [(jnp.arange(array.shape[axis_at]) // (array.shape[axis_at] // parts)).reshape([-1 if axis == axis_at else 1 for axis in range(array.ndim)]) for axis_at in (source, target)]
    chosen = jax.random.permutation(stream_key, parts)[partner]
    strong = (owner == chosen) | (owner == (partner + parts // 2) % parts)
    return jnp.where(strong, factor * array, array)


def steps_of(stream_key, dims, cuts, smallest, high):
    factor_of, own = 1.0, jax.random.fold_in(stream_key, 6)
    for dim, shards_of in cuts:
        heights = jnp.exp(jax.random.uniform(jax.random.fold_in(own, dim), (shards_of,), jnp.float32, smallest / len(cuts), high / len(cuts)))
        factor_of = factor_of * jnp.repeat(heights, dims[dim] // shards_of).reshape([-1 if axis == dim else 1 for axis in range(len(dims))])
    return factor_of


def noise_with(own_key, shape, spread, limit, cuts, heavy, held_as=jnp.bfloat16):
    array = spread * jax.random.normal(own_key, shape, jnp.float32)
    if cuts:
        array = array * steps_of(own_key, shape, cuts, -0.22, 0.18)
    return jnp.clip(with_spikes(array, jax.random.fold_in(own_key, 3), *heavy), -limit, limit).astype(held_as)


def setup_inputs(seed: int = 0) -> dict:
    key_of = jax.random.split(jax.random.key(seed), 7)
    return {
        "data_t": noise_with(key_of[0], (FEATURES, SAMPLES), FEATURES ** -0.5, 0.125, ((0, 32),), (1, 0, 32, 2.75)),
        "labels": draw_labels(jax.random.fold_in(key_of[6], 71), 0),
        "sample_weight": draw_sample_weight(jax.random.fold_in(key_of[6], 71), 0),
        "w_start": draw_w_start(jax.random.fold_in(key_of[6], 71), 0),
        "alpha_start": jnp.clip(1.0 * jax.random.uniform(key_of[4], (SAMPLES,), jnp.float32) ** steps_of(key_of[4], (SAMPLES,), ((0, 32),), -0.2, 0.2), 0.0, 1.0),
        "visit_order": jax.vmap(lambda own: jax.random.permutation(own, BLOCK))(jax.random.split(key_of[5], BLOCKS)).reshape((BLOCKS, BLOCK)).astype(jnp.int32),
    }


def sweep_rows(gram_block, label_rows, bound_rows, alpha_rows, margin_rows, visit_rows):
    gram_perm = gram_block[visit_rows][:, visit_rows]
    label_perm = label_rows[visit_rows]
    bound_perm = bound_rows[visit_rows]
    alpha_perm = alpha_rows[visit_rows]
    margin_perm = margin_rows[visit_rows]
    diag_perm = jnp.diagonal(gram_perm) + 1e-6

    def update_group(group_index, state_pair):
        alpha_now, margin_now = state_pair
        first_row = jnp.asarray(group_index * GROUP).astype(jnp.int32)
        group_alpha = lax.dynamic_slice_in_dim(alpha_now, first_row, GROUP)
        group_label = lax.dynamic_slice_in_dim(label_perm, first_row, GROUP)
        group_margin = lax.dynamic_slice_in_dim(margin_now, first_row, GROUP)
        group_diag = lax.dynamic_slice_in_dim(diag_perm, first_row, GROUP)
        group_bound = lax.dynamic_slice_in_dim(bound_perm, first_row, GROUP)
        fresh_alpha = jnp.clip(group_alpha + (1.0 - group_label * group_margin) / (2.0 * group_diag), 0.0, group_bound)
        change = fresh_alpha - group_alpha
        columns = lax.dynamic_slice_in_dim(gram_perm, first_row, GROUP, 1)
        margin_now = margin_now + 2.0 * jnp.dot(columns, group_label * change, precision=lax.Precision.HIGHEST)
        alpha_now = lax.dynamic_update_slice_in_dim(alpha_now, fresh_alpha, first_row, 0)
        return alpha_now, margin_now

    alpha_perm, margin_perm = lax.fori_loop(0, alpha_rows.shape[0] // GROUP, update_group, (alpha_perm, margin_perm))
    return jnp.zeros_like(alpha_rows).at[visit_rows].set(alpha_perm)


def reference(data_t, labels, sample_weight, w_start, alpha_start, visit_order):
    features, samples = data_t.shape
    devices = N_SHARD
    row_count = samples // devices
    label_sign = labels.astype(jnp.float32)
    start_margin = jnp.dot(w_start.astype(jnp.bfloat16), data_t, preferred_element_type=jnp.float32)
    weighted = (sample_weight * label_sign * jnp.maximum(0.0, 1.0 - label_sign * start_margin)).astype(jnp.bfloat16)
    ascent = jnp.dot(data_t, weighted, preferred_element_type=jnp.float32)
    column_sq = jnp.einsum("fs,fs->f", data_t, data_t, preferred_element_type=jnp.float32)
    scale_col = column_sq / samples + 1e-6
    stepped = w_start + ascent / (samples * scale_col)
    thresh = 1.0 / (4.0 * features * scale_col)
    primal = stepped - jnp.clip(stepped, -thresh, thresh)
    model_margin = jnp.dot(primal.astype(jnp.bfloat16), data_t, preferred_element_type=jnp.float32)
    objective = jnp.sum(sample_weight * jnp.square(jnp.maximum(0.0, 1.0 - label_sign * model_margin))) / (2.0 * samples) + jnp.sum(jnp.abs(primal)) / (4.0 * features)
    block_count = row_count // BLOCK
    visit_rows = visit_order.reshape(devices, block_count, BLOCK) + (jnp.arange(block_count, dtype=jnp.int32) * BLOCK)[None, :, None]
    visit_rows = visit_rows.reshape(devices, row_count).astype(jnp.int32)

    def gram_one(device_number):
        first = (device_number * row_count).astype(jnp.int32)
        piece = lax.dynamic_slice_in_dim(data_t, first, row_count, 1)
        return lax.dot_general(piece, piece, (((0,), (0,)), ((), ())), preferred_element_type=jnp.float32)

    gram_all = lax.map(gram_one, jnp.arange(devices, dtype=jnp.int32))
    sign_dev = label_sign.reshape(devices, row_count)
    bound_dev = sample_weight.reshape(devices, row_count)
    alpha_zero = bound_dev * alpha_start.reshape(devices, row_count)
    sweep_all = jax.vmap(sweep_rows)
    alpha_one = sweep_all(gram_all, sign_dev, bound_dev, alpha_zero, model_margin.reshape(devices, row_count), visit_rows)
    change_one = (sign_dev * (alpha_one - alpha_zero)).reshape(samples).astype(jnp.bfloat16)
    update_one = jnp.dot(data_t, change_one, preferred_element_type=jnp.float32) * (2.0 / devices)
    second_margin = model_margin + jnp.dot(update_one.astype(jnp.bfloat16), data_t, preferred_element_type=jnp.float32)
    alpha_two = sweep_all(gram_all, sign_dev, bound_dev, alpha_one, second_margin.reshape(devices, row_count), visit_rows)
    change_two = (sign_dev * (alpha_two - alpha_one)).reshape(samples).astype(jnp.bfloat16)
    update_two = jnp.dot(data_t, change_two, preferred_element_type=jnp.float32) * (2.0 / devices)
    weights_out = primal + update_one + update_two
    return weights_out, alpha_two.reshape(samples), objective
```

```python
import functools

import jax
import jax.numpy as jnp
from jax import lax
from jax.experimental import pallas as pl
from jax.experimental.pallas import tpu as pltpu
from jax.sharding import PartitionSpec as P

GROUP = 16
ROWS = 16
MESH = pl.DeviceIdType.MESH
F32 = jnp.float32
BF16 = jnp.bfloat16
HIGH = lax.Precision.HIGHEST


def nn(a, b, precision=None):
    return lax.dot_general(a, b, (((1,), (0,)), ((), ())), preferred_element_type=F32, precision=precision)


def nt(a, b, precision=None):
    return lax.dot_general(a, b, (((1,), (1,)), ((), ())), preferred_element_type=F32, precision=precision)


def spread(row):
    return jnp.broadcast_to(row, (ROWS, row.shape[-1])).astype(BF16)


def kernel(
    devices, data_hbm, label_hbm, bound_hbm, start_hbm, frac_hbm, visit_hbm,
    out_ref,
    part0, part1, part2, got0, got1, got2, own0, own1, own2, all0, all1, all2,
    data_ref, label_ref, bound_ref, start_ref, frac_ref, visit_ref, squares, gram, in_a, in_b, in_c, sum_a, sum_b, sum_c, gram_in,
    load_sem, small_sem, send_sem, recv_sem, gather_sem, send_a, recv_a, send_b, recv_b, send_c, recv_c, gram_send, gram_recv,
):
    me = lax.axis_index("shard")
    feats, samples = data_hbm.shape
    rows = label_hbm.shape[2]
    blocks, block = visit_hbm.shape
    features = feats * devices
    cubes = devices // 8
    cube = me // 8
    bit0, bit1, bit2 = me % 2, (me // 2) % 2, (me // 4) % 2
    partner = me + 1 - 2 * bit0

    def columns(k):
        return pl.ds(pl.multiple_of(k * rows, rows), rows)

    def loop(first, last, action):
        def step(i, carry):
            action(i)
            return carry

        lax.fori_loop(first, last, step, 0)

    upward = cube // (cubes // 2)

    def near(i):
        place = upward * (cubes - 2 - i) + (1 - upward) * i
        return place + jnp.where(place >= cube, 1, 0)

    def far(i):
        return near(cubes - 2 - i)

    def mates(action):
        loop(1, 8, lambda i: action(8 * cube + lax.rem(me + i, 8)))

    def cube_of(q, action):
        loop(0, 8, lambda j: action(8 * q + j))

    def peers(action):
        loop(0, cubes - 1, lambda i: cube_of(far(i), action))
        mates(action)

    def remote(source, target, send, recv, peer):
        return pltpu.make_async_remote_copy(
            src_ref=source, dst_ref=target, send_sem=send, recv_sem=recv,
            device_id=(peer,), device_id_type=MESH,
        )

    def total_wait(ref, phase):
        view = ref.at[pl.ds(0, devices - 1)]
        return remote(view, view, send_sem.at[phase], recv_sem.at[phase % 3], partner)

    def scatter_send(part, got, phase):
        def send(peer):
            remote(part.at[peer], got.at[me], send_sem.at[phase], recv_sem.at[phase], peer).start()

        return send

    def gather_start(own, everyone, phase):
        everyone[me] = own[...]
        spot = (phase - 3) * cubes + cube
        peers(lambda peer: remote(own, everyone.at[me], send_sem.at[phase], gather_sem.at[spot], peer).start())

    def part_of(lhs, part, q):
        for j in range(8):
            k = 8 * q + j
            part[k, 0:1, :] = nn(lhs, data_ref[:, columns(k)])[0:1, :]

    def margin_scatter(row, part, got, phase):
        lhs = spread(row)
        send = scatter_send(part, got, phase)

        def step(i):
            q = far(i)
            part_of(lhs, part, q)
            cube_of(q, send)

        loop(0, cubes - 1, step)
        part_of(lhs, part, cube)
        mates(send)
        got[me] = part[me]

    def back(everyone, phase, meanwhile=None):
        def arrival(q, count):
            view = everyone.at[pl.ds(8 * q, count)]
            spot = (phase - 3) * cubes + q
            remote(view, view, send_sem.at[phase], gather_sem.at[spot], partner).wait_recv()

        def cube_sum(q, total):
            for j in range(8):
                k = 8 * q + j
                total = total + nt(spread(everyone[k][0:1, 0:rows]), data_ref[:, columns(k)])
            return total

        def step(i, total):
            q = near(i)
            arrival(q, 8)
            return cube_sum(q, total)

        arrival(cube, 7)
        total = cube_sum(cube, jnp.zeros((ROWS, feats), F32))
        if meanwhile is not None:
            meanwhile()
        return lax.fori_loop(0, cubes - 1, step, total)[0:1, :]

    def load(q):
        view = pl.ds(pl.multiple_of(8 * q * rows, rows), 8 * rows)
        return pltpu.make_async_copy(data_hbm.at[:, view], data_ref.at[:, view], load_sem.at[q])

    small = [
        pltpu.make_async_copy(source, target, small_sem.at[i])
        for i, (source, target) in enumerate((
            (start_hbm, start_ref), (label_hbm.at[me], label_ref), (bound_hbm.at[me], bound_ref),
            (frac_hbm, frac_ref), (visit_hbm, visit_ref),
        ))
    ]
    small[0].start()
    loop(0, cubes - 1, lambda i: load(far(i)).start())
    load(cube).start()
    for copy in small[1:]:
        copy.start()
    barrier = pltpu.get_barrier_semaphore()
    peers(lambda peer: pl.semaphore_signal(barrier, inc=1, device_id=(peer,), device_id_type=MESH))

    row_at = lax.broadcasted_iota(jnp.int32, (block, block), 0)
    lane_at = lax.broadcasted_iota(jnp.int32, (block, block), 1)
    upper, lower, even = row_at < lane_at, row_at > lane_at, row_at == lane_at

    def gram_of(k):
        tile = data_ref[:, columns(k)]
        first, second = tile[:, :block], tile[:, block:]
        top = lax.dot_general(first, tile, (((0,), (0,)), ((), ())), preferred_element_type=F32)
        low = lax.dot_general(second, second, (((0,), (0,)), ((), ())), preferred_element_type=F32)
        gram[k, :, :block] = jnp.where(upper, top[:, :block], low).astype(BF16)
        gram[k, :, block:] = top[:, block:].astype(BF16)
        part1[k, 1:2, :block] = jnp.sum(jnp.where(even, top[:, :block], 0.0), axis=0, keepdims=True)
        part1[k, 1:2, block:] = jnp.sum(jnp.where(even, low, 0.0), axis=0, keepdims=True)

    def halving(source, target, index, sends, recvs, peer):
        return pltpu.make_async_remote_copy(
            src_ref=source, dst_ref=target.at[index], send_sem=sends.at[index],
            recv_sem=recvs.at[index], device_id=(peer,), device_id_type=MESH,
        )

    def copy_a(q, j):
        return halving(gram.at[8 * q + 2 * j + 1 - bit0], in_a, 4 * q + j, send_a, recv_a, partner)

    def order_of(i):
        swap = i % 2
        return (1 - swap) * bit1 + swap * bit2, 1 + swap, (1 - swap) * bit2 + swap * bit1, 2 - swap

    def copy_b(i, t):
        q = turn(i)
        bit, weight, _, other = order_of(i)
        return halving(
            sum_a.at[4 * q + weight * (1 - bit) + other * t], in_b, 2 * q + t, send_b, recv_b,
            me + 2 * weight * (1 - 2 * bit),
        )

    def copy_c(i):
        q = turn(i)
        _, _, bit, weight = order_of(i)
        return halving(sum_b.at[2 * q + 1 - bit], in_c, q, send_c, recv_c, me + 2 * weight * (1 - 2 * bit))

    def copy_d(q):
        return pltpu.make_async_remote_copy(
            src_ref=sum_c.at[q], dst_ref=gram_in.at[cube], send_sem=gram_send.at[0],
            recv_sem=gram_recv.at[0], device_id=(me + 8 * (q - cube),), device_id_type=MESH,
        )

    def added(x, y):
        return (x.astype(F32) + y.astype(F32)).astype(BF16)

    def turn(i):
        return jnp.where(i == cubes - 1, cube, far(jnp.minimum(i, cubes - 2)))

    def merge_a(i):
        q = turn(i)
        bit, weight, last, other = order_of(i)
        for t in (1 - last, last):
            for side in (1 - bit, bit):
                at = weight * side + other * t
                copy_a(q, at).wait_recv()
                sum_a[4 * q + at] = added(gram[8 * q + 2 * at + bit0], in_a[4 * q + at])
            copy_b(i, t).start()

    def merge_b(i):
        q = turn(i)
        bit, weight, last, other = order_of(i)
        for t in (1 - last, last):
            copy_b(i, t).wait_recv()
            sum_b[2 * q + t] = added(sum_a[4 * q + weight * bit + other * t], in_b[2 * q + t])
        copy_c(i).start()

    def merged_c(i):
        q = turn(i)
        bit = order_of(i)[2]
        copy_c(i).wait_recv()
        return added(sum_b[2 * q + bit], in_c[q])

    def merge_c(i):
        q = turn(i)
        sum_c[q] = merged_c(i)
        copy_d(q).start()

    def start_a(i):
        for j in range(4):
            copy_a(turn(i), j).start()

    def gram_part(i, side):
        for j in range(4):
            gram_of(8 * turn(i) + 2 * j + side)

    def gram_step(i):
        gram_part(i, 1 - bit0)
        start_a(i)
        gram_part(i, bit0)

    small[0].wait()
    w_start = start_ref[...]
    start_rows = spread(w_start)

    def add_squares(q):
        for r in range(0, feats, 32):
            total = squares[r:r + 32, :]
            for j in range(8 * blocks):
                at = pl.ds(pl.multiple_of(8 * q * rows + j * block, block), block)
                piece = data_ref[r:r + 32, at].astype(F32)
                total = total + piece * piece
            squares[r:r + 32, :] = total

    def first_part(q):
        load(q).wait()
        part_of(start_rows, part0, q)

    first_part(far(0))
    gram_part(0, 1 - bit0)
    gram_part(0, bit0)
    loop(1, cubes - 1, lambda i: first_part(far(i)))
    first_part(cube)
    pl.semaphore_wait(barrier, devices - 1)
    peers(scatter_send(part0, got0, 0))
    got0[me] = part0[me]
    start_a(0)

    def early_step(i):
        gram_step(i)
        merge_a(i - 1)

    loop(1, cubes - 1, early_step)
    gram_step(cubes - 1)
    squares[...] = jnp.zeros((feats, block), F32)
    loop(0, cubes, add_squares)
    for copy in small[1:]:
        copy.wait()
    sign, bound = label_ref[...].astype(F32), bound_ref[...]
    total_wait(got0, 0).wait_recv()
    margin0 = jnp.sum(got0[...], axis=0)
    own0[...] = bound * sign * jnp.maximum(0.0, 1.0 - sign * margin0)
    gather_start(own0, all0, 0 + 3)
    merge_a(cubes - 2)
    loop(0, cubes - 2, merge_b)
    merge_a(cubes - 1)
    square_total = squares[...]
    column_sq = nt(jnp.ones((8, block), F32), square_total, HIGH)[0:1, :]
    ascent = back(all0, 3)
    scale = column_sq / samples + 1e-06
    stepped = w_start + ascent / (samples * scale)
    thresh = 1.0 / (4.0 * features * scale)
    primal = stepped - jnp.clip(stepped, -thresh, thresh)
    margin_scatter(primal, part1, got1, 1)
    merge_b(cubes - 2)
    merge_c(0)
    merge_b(cubes - 1)
    loop(1, cubes - 1, merge_c)
    gram_in[cube] = merged_c(cubes - 1)

    orders, places = [], []
    for b in range(blocks):
        order = (lax.broadcasted_iota(jnp.int32, (block, block), 0) == visit_ref[b:b + 1, :]).astype(F32)
        orders.append(order)
        places.append(order.T.astype(BF16))

    alpha_zero = bound * frac_ref[...]

    def permute(vectors):
        stacked = jnp.concatenate(list(vectors) + [jnp.zeros((8 - len(vectors), rows), F32)], axis=0)
        return [nn(stacked[:, b * block:(b + 1) * block], orders[b], HIGH) for b in range(blocks)]

    total_wait(got1, 1).wait_recv()
    received = jnp.sum(got1[...], axis=0)
    margin1, diag = received[0:1, :], received[1:2, :]
    loss = jnp.sum(bound * jnp.square(jnp.maximum(0.0, 1.0 - sign * margin1)), axis=1, keepdims=True)
    penalty = jnp.sum(jnp.abs(primal), axis=1, keepdims=True)
    objective_part = loss / (2.0 * samples) + penalty / (4.0 * features)
    permuted = permute((sign, bound, alpha_zero, diag, margin1))
    sign_p = [x[0:1] for x in permuted]
    bound_p = [x[1:2] for x in permuted]
    zero_p = [x[2:3] for x in permuted]
    inverse_p = [0.5 / (x[3:4] + 1e-06) for x in permuted]
    margin_p = [x[4:5] for x in permuted]

    view = gram_in.at[pl.ds(0, cubes - 1)]
    gram_wait = pltpu.make_async_remote_copy(
        src_ref=view, dst_ref=view, send_sem=gram_send.at[0], recv_sem=gram_recv.at[0],
        device_id=(partner,), device_id_type=MESH,
    )
    gram_wait.wait_recv()
    full = jnp.sum(gram_in[...].astype(F32), axis=0)
    packed, cross = full[:, :block], full[:, block:]
    above, below = jnp.where(upper, packed, 0.0), jnp.where(lower, packed, 0.0)
    blocks_p = {}
    for (a, b), piece in {(0, 0): above + above.T, (0, 1): cross, (1, 1): below + below.T}.items():
        piece = nn(piece.astype(BF16), orders[b].astype(BF16)).astype(BF16)
        blocks_p[a, b] = nn(places[a], piece).astype(BF16)

    lane = lax.broadcasted_iota(jnp.int32, (1, block), 1)
    sub = lax.broadcasted_iota(jnp.int32, (ROWS, block), 0)

    def times_gram(delta, piece):
        high = delta.astype(BF16).astype(F32)
        lhs = jnp.where(sub == 0, high, jnp.where(sub == 1, delta - high, 0.0)).astype(BF16)
        return 2.0 * jnp.sum(nn(lhs, piece)[0:8], axis=0, keepdims=True)

    def sweep(alpha, margin):
        result, margin = [], list(margin)
        for b in range(blocks):
            now, m, moved = alpha[b], margin[b], jnp.zeros((1, block), F32)
            for s in range(block // GROUP):
                fresh = jnp.clip(now + (1.0 - sign_p[b] * m) * inverse_p[b], 0.0, bound_p[b])
                mine = (lane >= s * GROUP) & (lane < (s + 1) * GROUP)
                change = jnp.where(mine, fresh - now, 0.0)
                now = jnp.where(mine, fresh, now)
                change = sign_p[b] * change
                moved = moved + change
                if s + 1 < block // GROUP:
                    m = m + times_gram(change, blocks_p[b, b])
            for later in range(b + 1, blocks):
                margin[later] = margin[later] + times_gram(moved, blocks_p[b, later])
            result.append(now)
        return result

    def changes(after, before):
        pieces = []
        for b in range(blocks):
            z = spread(sign_p[b] * (after[b] - before[b]))
            pieces.append(nt(z, orders[b].astype(BF16))[0:1, :])
        return jnp.concatenate(pieces, axis=1)

    one_p = sweep(zero_p, margin_p)
    own1[0:1, 0:rows] = changes(one_p, zero_p)
    own1[0:1, rows:] = jnp.broadcast_to(objective_part, (1, block))
    gather_start(own1, all1, 1 + 3)
    update_one = back(all1, 4) * (2.0 / devices)
    margin_scatter(update_one, part2, got2, 2)
    out_ref[:, feats + rows:] = jnp.sum(all1[...], axis=0)[:, rows:]
    total_wait(got2, 2).wait_recv()
    margin2 = margin1 + jnp.sum(got2[...], axis=0)
    margin2_p = [x[0:1] for x in permute((margin2,))]
    two_p = sweep(one_p, margin2_p)
    own2[...] = changes(two_p, one_p)
    gather_start(own2, all2, 2 + 3)
    def alpha_out():
        for b in range(blocks):
            spot = jnp.broadcast_to(two_p[b], (8, block))
            out_ref[:, feats + b * block:feats + (b + 1) * block] = nt(spot, orders[b], HIGH)[0:1, :]

    out_ref[:, :feats] = primal + update_one + back(all2, 5, alpha_out) * (2.0 / devices)

    for phase, ref in enumerate((got0, got1, got2)):
        total_wait(ref, phase).wait_send()
    for phase, ref in enumerate((all0, all1, all2)):
        total_wait(ref, phase + 3).wait_send()
    gram_wait.wait_send()

    def drain(i):
        for j in range(4):
            copy_a(turn(i), j).wait_send()
        for j in range(2):
            copy_b(i, j).wait_send()
        copy_c(i).wait_send()

    loop(0, cubes, drain)


def split(packed, weights, alpha, objective):
    feats, rows = weights.shape[1], alpha.shape[1]
    weights[...] = packed[:, :feats]
    alpha[...] = packed[:, feats:feats + rows]
    objective[...] = packed[:, feats + rows:feats + rows + 1]


def body(devices, data_t, labels, sample_weight, w_start, alpha_start, visit_order):
    feats = data_t.shape[0]
    rows = alpha_start.shape[0]
    blocks, block = visit_order.shape
    cubes = devices // 8
    labels = labels.reshape(devices, 1, rows)
    bound = sample_weight.reshape(devices, 1, rows)

    def grams(count):
        return pltpu.VMEM((count, block, rows), BF16)

    def semaphores(count):
        return pltpu.SemaphoreType.DMA((count,))

    def vectors(height, length):
        return pltpu.VMEM((devices, height, length), F32)

    vmem = pl.BlockSpec(memory_space=pltpu.VMEM)
    out = pl.pallas_call(
        functools.partial(kernel, devices),
        name="svm_rounds",
        out_shape=jax.ShapeDtypeStruct((1, feats + rows + block), F32),
        in_specs=[pl.BlockSpec(memory_space=pl.ANY)] * 6,
        out_specs=vmem,
        scratch_shapes=[
            vectors(1, rows), vectors(2, rows), vectors(1, rows),
            vectors(1, rows), vectors(2, rows), vectors(1, rows),
            pltpu.VMEM((1, rows), F32), pltpu.VMEM((1, rows + block), F32), pltpu.VMEM((1, rows), F32),
            vectors(1, rows), vectors(1, rows + block), vectors(1, rows),
            pltpu.VMEM(data_t.shape, BF16), pltpu.VMEM((1, rows), jnp.int32), pltpu.VMEM((1, rows), F32),
            pltpu.VMEM((1, feats), F32), pltpu.VMEM((1, rows), F32), pltpu.VMEM((blocks, block), jnp.int32),
            pltpu.VMEM((feats, block), F32), grams(devices), grams(4 * cubes), grams(2 * cubes), grams(cubes),
            grams(4 * cubes), grams(2 * cubes), grams(cubes), grams(cubes),
            semaphores(cubes), semaphores(5), semaphores(6), semaphores(3), semaphores(3 * cubes), semaphores(4 * cubes), semaphores(4 * cubes),
            semaphores(2 * cubes), semaphores(2 * cubes), semaphores(cubes), semaphores(cubes),
            semaphores(1), semaphores(1),
        ],
        compiler_params=pltpu.CompilerParams(
            collective_id=0, has_side_effects=True, vmem_limit_bytes=63 * 1024 * 1024
        ),
    )(data_t, labels, bound, w_start[None], alpha_start[None], visit_order)
    weights, alpha, objective = pl.pallas_call(
        split,
        name="split",
        out_shape=(
            jax.ShapeDtypeStruct((1, feats), F32), jax.ShapeDtypeStruct((1, rows), F32), jax.ShapeDtypeStruct((1, 1), F32)
        ),
        in_specs=[vmem],
        out_specs=(vmem, vmem, vmem),
    )(out)
    return weights[0], alpha[0], objective[0, 0]


def solution(mesh):
    placed = (P("shard", None), P(), P(), P("shard"), P("shard"), P("shard", None))
    return jax.shard_map(
        functools.partial(body, mesh.shape["shard"]), mesh=mesh, in_specs=placed,
        out_specs=(P("shard"), P("shard"), P()), check_vma=False,
    )
```

```python
import functools

import jax
import jax.numpy as jnp
from jax import lax
from jax.experimental import pallas as pl
from jax.experimental.pallas import tpu as pltpu
from jax.sharding import PartitionSpec as P

GROUP = 16
ROWS = 16
MESH = pl.DeviceIdType.MESH
F32 = jnp.float32
BF16 = jnp.bfloat16
HIGH = lax.Precision.HIGHEST


def nn(a, b, precision=None):
    return lax.dot_general(a, b, (((1,), (0,)), ((), ())), preferred_element_type=F32, precision=precision)


def nt(a, b, precision=None):
    return lax.dot_general(a, b, (((1,), (1,)), ((), ())), preferred_element_type=F32, precision=precision)


def spread(row):
    return jnp.broadcast_to(row, (ROWS, row.shape[-1])).astype(BF16)


def kernel(
    devices, data_hbm, label_hbm, bound_hbm, label_tiles, bound_tiles, start_hbm, frac_hbm, visit_hbm,
    out_ref,
    part0, part1, part2, got0, got1, got2, own0, own1, own2, all0, all1, all2,
    data_ref, label_ref, bound_ref, owned_label, owned_bound, start_ref, frac_ref, visit_ref, squares, gram, in_a, in_b, in_c, sum_a, sum_b, sum_c, gram_in,
    picks, table, square, sign_c, bound_c, inverse_c, alpha_c, margin_c,
    load_sem, small_sem, send_sem, recv_sem, gather_sem, send_a, recv_a, send_b, recv_b, send_c, recv_c, gram_send, gram_recv,
):
    me = lax.axis_index("shard")
    feats, samples = data_hbm.shape
    rows = label_hbm.shape[2]
    blocks, block = visit_hbm.shape
    features = feats * devices
    cubes = devices // 8
    cube = me // 8
    bit0, bit1, bit2 = me % 2, (me // 2) % 2, (me // 4) % 2
    partner = me + 1 - 2 * bit0

    def columns(k):
        return pl.ds(pl.multiple_of(k * rows, rows), rows)

    def loop(first, last, action):
        def step(i, carry):
            action(i)
            return carry

        lax.fori_loop(first, last, step, 0)

    upward = cube // (cubes // 2)
    owners = label_tiles.shape[0]
    held = devices // owners
    low = cubes // 4
    is_owner = (cube >= low) & (cube < cubes - low) & (bit0 == 1)
    mine = jnp.clip(me // 2 - 4 * low, 0, owners - 1)

    def near(i):
        place = upward * (cubes - 2 - i) + (1 - upward) * i
        return place + jnp.where(place >= cube, 1, 0)

    def far(i):
        return near(cubes - 2 - i)

    def mates(action):
        loop(1, 8, lambda i: action(8 * cube + lax.rem(me + i, 8)))

    def cube_of(q, action):
        loop(0, 8, lambda j: action(8 * q + j))

    def peers(action):
        loop(0, cubes - 1, lambda i: cube_of(far(i), action))
        mates(action)

    def remote(source, target, send, recv, peer):
        return pltpu.make_async_remote_copy(
            src_ref=source, dst_ref=target, send_sem=send, recv_sem=recv,
            device_id=(peer,), device_id_type=MESH,
        )

    def total_wait(ref, phase):
        view = ref.at[pl.ds(0, devices - 1)]
        return remote(view, view, send_sem.at[phase], recv_sem.at[phase % 3], partner)

    def scatter_send(part, got, phase):
        def send(peer):
            remote(part.at[peer], got.at[me], send_sem.at[phase], recv_sem.at[phase], peer).start()

        return send

    def gather_start(own, everyone, phase):
        everyone[me] = own[...]
        spot = (phase - 3) * cubes + cube
        peers(lambda peer: remote(own, everyone.at[me], send_sem.at[phase], gather_sem.at[spot], peer).start())

    def part_of(lhs, part, q):
        for j in range(8):
            k = 8 * q + j
            part[k, 0:1, :] = nn(lhs, data_ref[:, columns(k)])[0:1, :]

    def margin_scatter(row, part, got, phase):
        lhs = spread(row)
        send = scatter_send(part, got, phase)

        def step(i):
            q = far(i)
            part_of(lhs, part, q)
            cube_of(q, send)

        loop(0, cubes - 1, step)
        part_of(lhs, part, cube)
        mates(send)
        got[me] = part[me]

    def back(everyone, phase, meanwhile=None):
        def arrival(q, count):
            view = everyone.at[pl.ds(8 * q, count)]
            spot = (phase - 3) * cubes + q
            remote(view, view, send_sem.at[phase], gather_sem.at[spot], partner).wait_recv()

        def cube_sum(q, total):
            for j in range(8):
                k = 8 * q + j
                total = total + nt(spread(everyone[k][0:1, 0:rows]), data_ref[:, columns(k)])
            return total

        def step(i, total):
            q = near(i)
            arrival(q, 8)
            return cube_sum(q, total)

        arrival(cube, 7)
        total = cube_sum(cube, jnp.zeros((ROWS, feats), F32))
        if meanwhile is not None:
            meanwhile()
        return lax.fori_loop(0, cubes - 1, step, total)[0:1, :]

    def load(q):
        view = pl.ds(pl.multiple_of(8 * q * rows, rows), 8 * rows)
        return pltpu.make_async_copy(data_hbm.at[:, view], data_ref.at[:, view], load_sem.at[q])

    small = [
        pltpu.make_async_copy(source, target, small_sem.at[i])
        for i, (source, target) in enumerate((
            (start_hbm, start_ref), (label_hbm.at[me], label_ref), (bound_hbm.at[me], bound_ref),
            (frac_hbm, frac_ref), (visit_hbm, visit_ref),
            (label_tiles.at[mine], owned_label), (bound_tiles.at[mine], owned_bound),
        ))
    ]
    small[0].start()
    loop(0, cubes - 1, lambda i: load(far(i)).start())
    load(cube).start()
    for copy in small[1:]:
        copy.start()
    barrier = pltpu.get_barrier_semaphore()
    peers(lambda peer: pl.semaphore_signal(barrier, inc=1, device_id=(peer,), device_id_type=MESH))

    row_at = lax.broadcasted_iota(jnp.int32, (block, block), 0)
    lane_at = lax.broadcasted_iota(jnp.int32, (block, block), 1)
    upper, lower, even = row_at < lane_at, row_at > lane_at, row_at == lane_at

    def gram_of(k):
        tile = data_ref[:, columns(k)]
        first, second = tile[:, :block], tile[:, block:]
        top = lax.dot_general(first, tile, (((0,), (0,)), ((), ())), preferred_element_type=F32)
        low = lax.dot_general(second, second, (((0,), (0,)), ((), ())), preferred_element_type=F32)
        gram[k, :, :block] = jnp.where(upper, top[:, :block], low).astype(BF16)
        gram[k, :, block:] = top[:, block:].astype(BF16)
        part1[k, 1:2, :block] = jnp.sum(jnp.where(even, top[:, :block], 0.0), axis=0, keepdims=True)
        part1[k, 1:2, block:] = jnp.sum(jnp.where(even, low, 0.0), axis=0, keepdims=True)

    def halving(source, target, index, sends, recvs, peer):
        return pltpu.make_async_remote_copy(
            src_ref=source, dst_ref=target.at[index], send_sem=sends.at[index],
            recv_sem=recvs.at[index], device_id=(peer,), device_id_type=MESH,
        )

    def copy_a(q, j):
        return halving(gram.at[8 * q + 2 * j + 1 - bit0], in_a, 4 * q + j, send_a, recv_a, partner)

    def order_of(i):
        swap = i % 2
        return (1 - swap) * bit1 + swap * bit2, 1 + swap, (1 - swap) * bit2 + swap * bit1, 2 - swap

    def copy_b(i, t):
        q = turn(i)
        bit, weight, _, other = order_of(i)
        return halving(
            sum_a.at[4 * q + weight * (1 - bit) + other * t], in_b, 2 * q + t, send_b, recv_b,
            me + 2 * weight * (1 - 2 * bit),
        )

    def copy_c(i):
        q = turn(i)
        _, _, bit, weight = order_of(i)
        return halving(sum_b.at[2 * q + 1 - bit], in_c, q, send_c, recv_c, me + 2 * weight * (1 - 2 * bit))

    def copy_d(q, half):
        view = pl.ds(half * block, block)
        return pltpu.make_async_remote_copy(
            src_ref=sum_c.at[q, :, view], dst_ref=gram_in.at[cube, :, view], send_sem=gram_send.at[half],
            recv_sem=gram_recv.at[half], device_id=(me + 8 * (q - cube),), device_id_type=MESH,
        )

    def wait_d(half):
        view = gram_in.at[pl.ds(0, cubes - 1), :, pl.ds(half * block, block)]
        return pltpu.make_async_remote_copy(
            src_ref=view, dst_ref=view, send_sem=gram_send.at[half], recv_sem=gram_recv.at[half],
            device_id=(partner,), device_id_type=MESH,
        )

    def added(x, y):
        return (x.astype(F32) + y.astype(F32)).astype(BF16)

    def turn(i):
        return jnp.where(i == cubes - 1, cube, far(jnp.minimum(i, cubes - 2)))

    def merge_a(i):
        q = turn(i)
        bit, weight, last, other = order_of(i)
        for t in (1 - last, last):
            for side in (1 - bit, bit):
                at = weight * side + other * t
                copy_a(q, at).wait_recv()
                sum_a[4 * q + at] = added(gram[8 * q + 2 * at + bit0], in_a[4 * q + at])
            copy_b(i, t).start()

    def merge_b(i):
        q = turn(i)
        bit, weight, last, other = order_of(i)
        for t in (1 - last, last):
            copy_b(i, t).wait_recv()
            sum_b[2 * q + t] = added(sum_a[4 * q + weight * bit + other * t], in_b[2 * q + t])
        copy_c(i).start()

    def merged_c(i):
        q = turn(i)
        bit = order_of(i)[2]
        copy_c(i).wait_recv()
        return added(sum_b[2 * q + bit], in_c[q])

    def merge_c(i):
        q = turn(i)
        sum_c[q] = merged_c(i)
        copy_d(q, 0).start()
        copy_d(q, 1).start()

    def start_a(i):
        for j in range(4):
            copy_a(turn(i), j).start()

    def gram_part(i, side):
        for j in range(4):
            gram_of(8 * turn(i) + 2 * j + side)

    def gram_step(i):
        gram_part(i, 1 - bit0)
        start_a(i)
        gram_part(i, bit0)

    small[0].wait()
    w_start = start_ref[...]
    start_rows = spread(w_start)

    def add_squares(q):
        for r in range(0, feats, 32):
            total = squares[r:r + 32, :]
            for j in range(8 * blocks):
                at = pl.ds(pl.multiple_of(8 * q * rows + j * block, block), block)
                piece = data_ref[r:r + 32, at].astype(F32)
                total = total + piece * piece
            squares[r:r + 32, :] = total

    def first_part(q):
        load(q).wait()
        for j in range(8):
            row = nn(start_rows, data_ref[:, columns(8 * q + j)])
            for b in range(blocks):
                at = j % held * blocks + b
                part0[8 // held * q + j // held, at:at + 1, :] = row[0:1, b * block:(b + 1) * block]

    def each_owner(action):
        def step(i):
            o = upward * i + (1 - upward) * (owners - 1 - i)
            peer = 8 * low + 2 * o + 1

            @pl.when(peer != me)
            def _():
                action(o, peer)

        loop(0, owners, step)

    def owned(ref, count):
        return ref.at[pl.ds(0, count)]

    def waiting(ref, count, send, recv):
        view = owned(ref, count)
        return remote(view, view, send, recv, partner)

    first_part(far(0))
    gram_part(0, 1 - bit0)
    gram_part(0, bit0)
    loop(1, cubes - 1, lambda i: first_part(far(i)))
    first_part(cube)
    pl.semaphore_wait(barrier, devices - 1)
    each_owner(lambda o, peer: remote(part0.at[o], got0.at[me], send_sem.at[0], recv_sem.at[0], peer).start())
    start_a(0)

    def early_step(i):
        gram_step(i)
        merge_a(i - 1)

    loop(1, cubes - 1, early_step)
    gram_step(cubes - 1)
    squares[...] = jnp.zeros((feats, block), F32)
    loop(0, cubes, add_squares)
    for copy in small[1:]:
        copy.wait()
    sign, bound = label_ref[...].astype(F32), bound_ref[...]

    @pl.when(is_owner)
    def _():
        got0[me] = part0[mine]
        waiting(got0, devices - 1, send_sem.at[0], recv_sem.at[0]).wait_recv()
        margin0 = jnp.sum(got0[...], axis=0)
        side = owned_label[...].astype(F32)
        own0[...] = (owned_bound[...] * side * jnp.maximum(0.0, 1.0 - side * margin0)).astype(BF16)
        all0[mine] = own0[...]
        peers(lambda peer: remote(own0, all0.at[mine], send_sem.at[3], gather_sem.at[cube], peer).start())

    merge_a(cubes - 2)
    loop(0, cubes - 2, merge_b)
    merge_a(cubes - 1)
    square_total = squares[...]
    column_sq = nt(jnp.ones((8, block), F32), square_total, HIGH)[0:1, :]
    def start_sum(i, total):
        q = low + upward * (cubes - 2 * low - 1 - i) + (1 - upward) * i

        def wait(count):
            view = all0.at[pl.ds(0, count)]
            remote(view, view, send_sem.at[3], gather_sem.at[q], partner).wait_recv()

        own_turn = is_owner & (q == cube)

        @pl.when(own_turn)
        def _():
            wait(3)

        @pl.when(jnp.logical_not(own_turn))
        def _():
            wait(4)

        for j in range(4):
            o = 4 * (q - low) + j
            vector = all0[o].astype(F32)
            for b in range(held):
                row = jnp.concatenate([vector[b * blocks + c:b * blocks + c + 1] for c in range(blocks)], axis=1)
                total = total + nt(spread(row), data_ref[:, columns(held * o + b)])
        return total

    ascent = lax.fori_loop(0, cubes - 2 * low, start_sum, jnp.zeros((ROWS, feats), F32))[0:1, :]
    scale = column_sq / samples + 1e-06
    stepped = w_start + ascent / (samples * scale)
    thresh = 1.0 / (4.0 * features * scale)
    primal = stepped - jnp.clip(stepped, -thresh, thresh)
    margin_scatter(primal, part1, got1, 1)
    merge_b(cubes - 2)
    merge_c(0)
    merge_b(cubes - 1)
    loop(1, cubes - 1, merge_c)
    gram_in[cube] = merged_c(cubes - 1)

    orders, places = [], []
    for b in range(blocks):
        order = (lax.broadcasted_iota(jnp.int32, (block, block), 0) == visit_ref[b:b + 1, :]).astype(F32)
        orders.append(order)
        places.append(order.T.astype(BF16))

    orders_half = [order.astype(BF16) for order in orders]
    twice = [jnp.concatenate([place, place], axis=1) for place in places]

    def upright(row, b):
        piece = row[:, b * block:(b + 1) * block]
        high = piece.astype(BF16).astype(F32)
        both = jnp.broadcast_to(jnp.concatenate([high, piece - high], axis=1), (block, 2 * block))
        return nt(twice[b], both.astype(BF16))

    alpha_zero = bound * frac_ref[...]
    for b in range(blocks):
        sign_c[b] = upright(sign, b)
        bound_c[b] = upright(bound, b)
        alpha_c[b] = upright(alpha_zero, b)
    pick_row = lax.broadcasted_iota(jnp.int32, (block, 2 * block), 0) % GROUP
    pick_lane = lax.broadcasted_iota(jnp.int32, (block, 2 * block), 1) // block
    for r in range(GROUP // 2):
        picks[r] = (pick_row == pick_lane + 2 * r).astype(F32).astype(BF16)

    total_wait(got1, 1).wait_recv()
    received = jnp.sum(got1[...], axis=0)
    margin1, diag = received[0:1, :], received[1:2, :]
    loss = jnp.sum(bound * jnp.square(jnp.maximum(0.0, 1.0 - sign * margin1)), axis=1, keepdims=True)
    penalty = jnp.sum(jnp.abs(primal), axis=1, keepdims=True)
    objective_part = loss / (2.0 * samples) + penalty / (4.0 * features)
    inverse = 0.5 / (diag + 1e-06)
    for b in range(blocks):
        inverse_c[b] = upright(inverse, b)
        margin_c[b] = upright(margin1, b)

    wait_d(0).wait_recv()
    packed = jnp.sum(gram_in[:, :, :block].astype(F32), axis=0)
    above, below = jnp.where(upper, packed, 0.0), jnp.where(lower, packed, 0.0)
    gap = row_at // GROUP - lane_at // GROUP

    def visited(a, b, piece):
        piece = nn(piece.astype(BF16), orders_half[b]).astype(BF16)
        return nn(places[a], piece)

    for b, piece in enumerate((above + above.T, below + below.T)):
        whole = visited(b, b, piece)
        square[b] = whole
        lagged = [jnp.where(gap == lag, whole, 0.0)[lag * GROUP:] for lag in (1, 2)]
        lagged = jnp.concatenate(lagged, axis=0).astype(BF16)
        for r in range(GROUP // 2):
            spots = nn(lagged, picks[r])
            for c in range(2):
                half = spots[:, c * block:(c + 1) * block]
                table[0, b, 2 * r + c, GROUP:, :] = half[:block - GROUP]
                table[1, b, 2 * r + c, 2 * GROUP:, :] = half[block - GROUP:]
    wait_d(1).wait_recv()
    between = visited(0, 1, jnp.sum(gram_in[:, :, block:].astype(F32), axis=0))
    sub = lax.broadcasted_iota(jnp.int32, (GROUP, block), 0)
    lane = lax.broadcasted_iota(jnp.int32, (GROUP, block), 1)

    def fold(x):
        return x[0:8] + x[8:16]

    def total_of(terms):
        while len(terms) > 1:
            terms = [sum(terms[i:i + 2]) for i in range(0, len(terms), 2)]
        return terms[0]

    def sweep():
        sets, offset, moves = block // GROUP, None, []
        for b in range(blocks):
            seen, passed, moved = [jnp.zeros((8, block), F32) for _ in range(3)]
            extra = [[] for _ in range(sets)]
            for s in range(sets):
                at = slice(s * GROUP, (s + 1) * GROUP)
                m = margin_c[b, at]
                if offset is not None:
                    m = m + offset[at]
                for term in extra[s]:
                    m = m + term
                now, side = alpha_c[b, at], sign_c[b, at]
                fresh = jnp.clip(now + (1.0 - side * m) * inverse_c[b, at], 0.0, bound_c[b, at])
                change = side * (fresh - now)
                alpha_c[b, at] = fresh
                moved = moved + fold(jnp.where(lane == sub + s * GROUP, change, 0.0))
                push = 2.0 * change
                steps = [jnp.broadcast_to(push[r:r + 1], (GROUP, block)) for r in range(GROUP)]
                if s + 3 < sets:
                    seen = seen + fold(push * square[b, at])
                    row = jnp.sum(seen, axis=0, keepdims=True)
                    spot = jnp.where(lane == sub + (s + 3) * GROUP, row, 0.0)
                    extra[s + 3].append(jnp.sum(spot, axis=1, keepdims=True))
                for lag in (2, 1):
                    if s + lag < sets:
                        there = slice((s + lag) * GROUP, (s + lag + 1) * GROUP)
                        extra[s + lag].append(
                            total_of([steps[r] * table[lag - 1, b, r, there] for r in range(GROUP)])
                        )
                if b + 1 < blocks:
                    passed = passed + fold(push * between[at])
            moves.append(jnp.sum(moved, axis=0, keepdims=True))
            if b + 1 < blocks:
                row = jnp.sum(passed, axis=0, keepdims=True)
                offset = jnp.sum(jnp.where(even, row, 0.0), axis=1, keepdims=True)
        return jnp.concatenate([nt(spread(x), orders_half[b])[0:1, :] for b, x in enumerate(moves)], axis=1)

    own1[0:1, 0:rows] = sweep()
    own1[0:1, rows:] = jnp.broadcast_to(objective_part, (1, block))
    gather_start(own1, all1, 1 + 3)
    update_one = back(all1, 4) * (2.0 / devices)
    margin_scatter(update_one, part2, got2, 2)
    out_ref[:, feats + rows:] = jnp.sum(all1[...], axis=0)[:, rows:]
    total_wait(got2, 2).wait_recv()
    margin2 = margin1 + jnp.sum(got2[...], axis=0)
    for b in range(blocks):
        margin_c[b] = upright(margin2, b)
    own2[...] = sweep()
    gather_start(own2, all2, 2 + 3)
    def alpha_out():
        for b in range(blocks):
            spot = jnp.broadcast_to(jnp.sum(jnp.where(even, alpha_c[b], 0.0), axis=0, keepdims=True), (8, block))
            out_ref[:, feats + b * block:feats + (b + 1) * block] = nt(spot, orders[b], HIGH)[0:1, :]

    out_ref[:, :feats] = primal + update_one + back(all2, 5, alpha_out) * (2.0 / devices)

    for phase, ref in ((1, got1), (2, got2), (4, all1), (5, all2)):
        total_wait(ref, phase).wait_send()

    @pl.when(is_owner)
    def _():
        waiting(part0, owners - 1, send_sem.at[0], recv_sem.at[0]).wait_send()
        def sent(_):
            remote(own0, all0.at[0], send_sem.at[3], recv_sem.at[0], partner).wait_send()

        loop(0, devices - 1, sent)

    @pl.when(jnp.logical_not(is_owner))
    def _():
        waiting(part0, owners, send_sem.at[0], recv_sem.at[0]).wait_send()

    wait_d(0).wait_send()
    wait_d(1).wait_send()

    def drain(i):
        for j in range(4):
            copy_a(turn(i), j).wait_send()
        for j in range(2):
            copy_b(i, j).wait_send()
        copy_c(i).wait_send()

    loop(0, cubes, drain)


def split(packed, weights, alpha, objective):
    feats, rows = weights.shape[1], alpha.shape[1]
    weights[...] = packed[:, :feats]
    alpha[...] = packed[:, feats:feats + rows]
    objective[...] = packed[:, feats + rows:feats + rows + 1]


def body(devices, data_t, labels, sample_weight, w_start, alpha_start, visit_order):
    feats = data_t.shape[0]
    rows = alpha_start.shape[0]
    blocks, block = visit_order.shape
    cubes = devices // 8
    owners = cubes // 2 * 4
    span = (devices // owners * blocks, block)
    tiles = [x.reshape(owners, *span) for x in (labels, sample_weight)]
    labels = labels.reshape(devices, 1, rows)
    bound = sample_weight.reshape(devices, 1, rows)

    def grams(count):
        return pltpu.VMEM((count, block, rows), BF16)

    def semaphores(count):
        return pltpu.SemaphoreType.DMA((count,))

    def vectors(height, length):
        return pltpu.VMEM((devices, height, length), F32)

    vmem = pl.BlockSpec(memory_space=pltpu.VMEM)
    out = pl.pallas_call(
        functools.partial(kernel, devices),
        name="svm_rounds",
        out_shape=jax.ShapeDtypeStruct((1, feats + rows + block), F32),
        in_specs=[pl.BlockSpec(memory_space=pl.ANY)] * 8,
        out_specs=vmem,
        scratch_shapes=[
            pltpu.VMEM((owners, *span), F32), vectors(2, rows), vectors(1, rows),
            pltpu.VMEM((devices, *span), F32), vectors(2, rows), vectors(1, rows),
            pltpu.VMEM(span, BF16), pltpu.VMEM((1, rows + block), F32), pltpu.VMEM((1, rows), F32),
            pltpu.VMEM((owners, *span), BF16), vectors(1, rows + block), vectors(1, rows),
            pltpu.VMEM(data_t.shape, BF16), pltpu.VMEM((1, rows), jnp.int32), pltpu.VMEM((1, rows), F32),
            pltpu.VMEM(span, jnp.int32), pltpu.VMEM(span, F32),
            pltpu.VMEM((1, feats), F32), pltpu.VMEM((1, rows), F32), pltpu.VMEM((blocks, block), jnp.int32),
            pltpu.VMEM((feats, block), F32), grams(devices), grams(4 * cubes), grams(2 * cubes), grams(cubes),
            grams(4 * cubes), grams(2 * cubes), grams(cubes), grams(cubes),
            pltpu.VMEM((GROUP // 2, block, 2 * block), BF16), pltpu.VMEM((2, blocks, GROUP, block, block), F32),
            *[pltpu.VMEM((blocks, block, block), F32)] * 6,
            semaphores(cubes), semaphores(7), semaphores(6), semaphores(3), semaphores(3 * cubes), semaphores(4 * cubes), semaphores(4 * cubes),
            semaphores(2 * cubes), semaphores(2 * cubes), semaphores(cubes), semaphores(cubes),
            semaphores(2), semaphores(2),
        ],
        compiler_params=pltpu.CompilerParams(
            collective_id=0, has_side_effects=True, vmem_limit_bytes=63 * 1024 * 1024
        ),
    )(data_t, labels, bound, *tiles, w_start[None], alpha_start[None], visit_order)
    weights, alpha, objective = pl.pallas_call(
        split,
        name="split",
        out_shape=(
            jax.ShapeDtypeStruct((1, feats), F32), jax.ShapeDtypeStruct((1, rows), F32), jax.ShapeDtypeStruct((1, 1), F32)
        ),
        in_specs=[vmem],
        out_specs=(vmem, vmem, vmem),
    )(out)
    return weights[0], alpha[0], objective[0, 0]


def solution(mesh):
    placed = (P("shard", None), P(), P(), P("shard"), P("shard"), P("shard", None))
    return jax.shard_map(
        functools.partial(body, mesh.shape["shard"]), mesh=mesh, in_specs=placed,
        out_specs=(P("shard"), P("shard"), P()), check_vma=False,
    )
```

```python
import functools

import jax
import jax.numpy as jnp
from jax import lax
from jax.experimental import pallas as pl
from jax.experimental.pallas import tpu as pltpu
from jax.sharding import PartitionSpec as P

GROUP = 16
ROWS = 16
MESH = pl.DeviceIdType.MESH
F32 = jnp.float32
BF16 = jnp.bfloat16
HIGH = lax.Precision.HIGHEST


def nn(a, b, precision=None):
    return lax.dot_general(a, b, (((1,), (0,)), ((), ())), preferred_element_type=F32, precision=precision)


def nt(a, b, precision=None):
    return lax.dot_general(a, b, (((1,), (1,)), ((), ())), preferred_element_type=F32, precision=precision)


def spread(row):
    return jnp.broadcast_to(row, (ROWS, row.shape[-1])).astype(BF16)


def kernel(
    devices, data_hbm, label_hbm, bound_hbm, label_tiles, bound_tiles, start_hbm, frac_hbm, visit_hbm,
    out_ref,
    part0, part1, part2, part_d, got0, got1, got2, got_d, own0, own1, own2, own_o, all0, all1, all2, all_o,
    data_ref, turned_ref, label_ref, bound_ref, owned_label, owned_bound, start_ref, frac_ref, visit_ref, squares, gram, in_a, in_b, in_c, sum_a, sum_b, sum_c, gram_in,
    picks, table, between_c, square, sign_c, bound_c, inverse_c, alpha_c, margin_c,
    load_sem, small_sem, send_sem, recv_sem, gather_sem, send_a, recv_a, send_b, recv_b, send_c, recv_c, gram_send, gram_recv,
):
    me = lax.axis_index("shard")
    feats, samples = data_hbm.shape
    rows = label_hbm.shape[2]
    blocks, block = visit_hbm.shape
    features = feats * devices
    cubes = devices // 8
    cube = me // 8
    bit0, bit1, bit2 = me % 2, (me // 2) % 2, (me // 4) % 2
    partner = me + 1 - 2 * bit0

    def columns(k):
        return pl.ds(pl.multiple_of(k * rows, rows), rows)

    def loop(first, last, action):
        def step(i, carry):
            action(i)
            return carry

        lax.fori_loop(first, last, step, 0)

    upward = cube // (cubes // 2)
    owners = label_tiles.shape[0]
    held = devices // owners
    low = cubes // 4
    is_owner = (cube >= low) & (cube < cubes - low) & (bit0 == 1)
    mine = jnp.clip(me // 2 - 4 * low, 0, owners - 1)

    def near(i):
        place = upward * (cubes - 2 - i) + (1 - upward) * i
        return place + jnp.where(place >= cube, 1, 0)

    def far(i):
        return near(cubes - 2 - i)

    def mates(action):
        loop(1, 8, lambda i: action(8 * cube + lax.rem(me + i, 8)))

    def cube_of(q, action):
        loop(0, 8, lambda j: action(8 * q + j))

    def peers(action):
        loop(0, cubes - 1, lambda i: cube_of(far(i), action))
        mates(action)

    def remote(source, target, send, recv, peer):
        return pltpu.make_async_remote_copy(
            src_ref=source, dst_ref=target, send_sem=send, recv_sem=recv,
            device_id=(peer,), device_id_type=MESH,
        )

    def total_wait(ref, phase):
        view = ref.at[pl.ds(0, devices - 1)]
        return remote(view, view, send_sem.at[phase], recv_sem.at[phase % 3 if phase < 6 else phase - 3], partner)

    def scatter_send(part, got, phase):
        def send(peer):
            arrived = recv_sem.at[phase if phase < 3 else phase - 3]
            remote(part.at[peer], got.at[me], send_sem.at[phase], arrived, peer).start()

        return send

    def gather_start(own, everyone, phase):
        everyone[me] = own[...]
        spot = (phase - 3) * cubes + cube
        peers(lambda peer: remote(own, everyone.at[me], send_sem.at[phase], gather_sem.at[spot], peer).start())

    def part_of(lhs, part, q):
        for j in range(8):
            k = 8 * q + j
            part[k, 0:1, :] = nn(lhs, data_ref[:, columns(k)])[0:1, :]

    def margin_scatter(row, part, got, phase):
        lhs = spread(row)
        send = scatter_send(part, got, phase)

        def step(i):
            q = far(i)
            part_of(lhs, part, q)
            cube_of(q, send)

        loop(0, cubes - 1, step)
        part_of(lhs, part, cube)
        mates(send)
        got[me] = part[me]

    def back(everyone, phase, meanwhile=None):
        def arrival(q, count):
            view = everyone.at[pl.ds(8 * q, count)]
            spot = (phase - 3) * cubes + q
            remote(view, view, send_sem.at[phase], gather_sem.at[spot], partner).wait_recv()

        def cube_sum(q, total):
            for j in range(8):
                k = 8 * q + j
                vector = everyone[k].astype(F32)
                row = jnp.concatenate([vector[b:b + 1] for b in range(blocks)], axis=1)
                total = total + nn(spread(row), turned_ref[k])
            return total

        def step(i, total):
            q = near(i)
            arrival(q, 8)
            return cube_sum(q, total)

        arrival(cube, 7)
        total = cube_sum(cube, jnp.zeros((ROWS, feats), F32))
        if meanwhile is not None:
            meanwhile()
        return lax.fori_loop(0, cubes - 1, step, total)[0:1, :]

    def load(q):
        view = pl.ds(pl.multiple_of(8 * q * rows, rows), 8 * rows)
        return pltpu.make_async_copy(data_hbm.at[:, view], data_ref.at[:, view], load_sem.at[q])

    small = [
        pltpu.make_async_copy(source, target, small_sem.at[i])
        for i, (source, target) in enumerate((
            (start_hbm, start_ref), (label_hbm.at[me], label_ref), (bound_hbm.at[me], bound_ref),
            (frac_hbm, frac_ref), (visit_hbm, visit_ref),
            (label_tiles.at[mine], owned_label), (bound_tiles.at[mine], owned_bound),
        ))
    ]
    small[0].start()
    loop(0, cubes - 1, lambda i: load(far(i)).start())
    load(cube).start()
    for copy in small[1:]:
        copy.start()
    barrier = pltpu.get_barrier_semaphore()
    peers(lambda peer: pl.semaphore_signal(barrier, inc=1, device_id=(peer,), device_id_type=MESH))

    row_at = lax.broadcasted_iota(jnp.int32, (block, block), 0)
    lane_at = lax.broadcasted_iota(jnp.int32, (block, block), 1)
    upper, lower, even = row_at < lane_at, row_at > lane_at, row_at == lane_at

    def gram_of(k):
        tile = data_ref[:, columns(k)]
        first, second = tile[:, :block], tile[:, block:]
        turned = tile.T
        turned_ref[k] = turned
        top, low = nn(turned[:block], tile), nn(turned[block:], second)
        gram[k, 0] = jnp.where(upper, top[:, :block], low).astype(BF16)
        gram[k, 1] = top[:, block:].astype(BF16)
        part_d[k, 0:1, :block] = jnp.sum(jnp.where(even, top[:, :block], 0.0), axis=0, keepdims=True)
        part_d[k, 0:1, block:] = jnp.sum(jnp.where(even, low, 0.0), axis=0, keepdims=True)

    def halving(source, target, index, sends, recvs, peer):
        return pltpu.make_async_remote_copy(
            src_ref=source, dst_ref=target, send_sem=sends.at[index],
            recv_sem=recvs.at[index], device_id=(peer,), device_id_type=MESH,
        )

    def copy_a(q, j):
        return halving(gram.at[8 * q + 2 * j + 1 - bit0], in_a.at[4 * q + j], 4 * q + j, send_a, recv_a, partner)

    orders_of = ((bit1, 1, bit2, 2), (bit2, 2, bit1, 1))

    def copy_b(i, t, half):
        q = turn(i)
        bit, weight, _, other = orders_of[half]
        return halving(
            sum_a.at[4 * q + weight * (1 - bit) + other * t, half], in_b.at[2 * q + t, half],
            4 * q + 2 * t + half, send_b, recv_b, me + 2 * weight * (1 - 2 * bit),
        )

    def copy_c(i, half):
        q = turn(i)
        _, _, bit, weight = orders_of[half]
        return halving(
            sum_b.at[2 * q + 1 - bit, half], in_c.at[q, half],
            2 * q + half, send_c, recv_c, me + 2 * weight * (1 - 2 * bit),
        )

    def copy_d(q, half):
        return pltpu.make_async_remote_copy(
            src_ref=sum_c.at[q, half], dst_ref=gram_in.at[cube, half], send_sem=gram_send.at[half],
            recv_sem=gram_recv.at[half], device_id=(me + 8 * (q - cube),), device_id_type=MESH,
        )

    def wait_d(half):
        view = gram_in.at[pl.ds(0, cubes - 1), half]
        return pltpu.make_async_remote_copy(
            src_ref=view, dst_ref=view, send_sem=gram_send.at[half], recv_sem=gram_recv.at[half],
            device_id=(partner,), device_id_type=MESH,
        )

    def added(x, y):
        return (x.astype(F32) + y.astype(F32)).astype(BF16)

    def turn(i):
        return jnp.where(i == cubes - 1, cube, far(jnp.minimum(i, cubes - 2)))

    def merge_a(i):
        q = turn(i)
        for j in range(4):
            copy_a(q, j).wait_recv()
            sum_a[4 * q + j] = added(gram[8 * q + 2 * j + bit0], in_a[4 * q + j])
        for half in range(2):
            for t in (1 - orders_of[half][2], orders_of[half][2]):
                copy_b(i, t, half).start()

    def merge_b(i):
        q = turn(i)
        for half in range(2):
            bit, weight, last, other = orders_of[half]
            for t in (1 - last, last):
                copy_b(i, t, half).wait_recv()
                sum_b[2 * q + t, half] = added(
                    sum_a[4 * q + weight * bit + other * t, half], in_b[2 * q + t, half]
                )
            copy_c(i, half).start()

    def merged_c(i, half):
        q = turn(i)
        copy_c(i, half).wait_recv()
        return added(sum_b[2 * q + orders_of[half][2], half], in_c[q, half])

    def merge_c(i):
        q = turn(i)
        for half in range(2):
            sum_c[q, half] = merged_c(i, half)
        copy_d(q, 0).start()

    def merge_x(i):
        copy_d(turn(i), 1).start()

    def start_a(i):
        for j in range(4):
            copy_a(turn(i), j).start()

    def gram_part(i, side):
        for j in range(4):
            gram_of(8 * turn(i) + 2 * j + side)

    def gram_step(i):
        gram_part(i, 1 - bit0)
        start_a(i)
        gram_part(i, bit0)

    small[0].wait()
    w_start = start_ref[...]
    start_rows = spread(w_start)

    def add_squares(q):
        for r in range(0, feats, 32):
            total = squares[r:r + 32, :]
            for j in range(8 * blocks):
                at = pl.ds(pl.multiple_of(8 * q * rows + j * block, block), block)
                piece = data_ref[r:r + 32, at].astype(F32)
                total = total + piece * piece
            squares[r:r + 32, :] = total

    def first_part(q):
        load(q).wait()
        for j in range(8):
            row = nn(start_rows, data_ref[:, columns(8 * q + j)])
            for b in range(blocks):
                at = j % held * blocks + b
                part0[8 // held * q + j // held, at:at + 1, :] = row[0:1, b * block:(b + 1) * block]

    def each_owner(action):
        def step(i):
            o = upward * i + (1 - upward) * (owners - 1 - i)
            peer = 8 * low + 2 * o + 1

            @pl.when(peer != me)
            def _():
                action(o, peer)

        loop(0, owners, step)

    def owned(ref, count):
        return ref.at[pl.ds(0, count)]

    def waiting(ref, count, send, recv):
        view = owned(ref, count)
        return remote(view, view, send, recv, partner)

    first_part(far(0))
    gram_part(0, 1 - bit0)
    gram_part(0, bit0)
    loop(1, cubes - 1, lambda i: first_part(far(i)))
    first_part(cube)
    pl.semaphore_wait(barrier, devices - 1)
    each_owner(lambda o, peer: remote(part0.at[o], got0.at[me], send_sem.at[0], recv_sem.at[0], peer).start())
    start_a(0)

    def early_step(i):
        gram_step(i)
        merge_a(i - 1)

    loop(1, cubes - 1, early_step)
    gram_step(cubes - 1)
    squares[...] = jnp.zeros((feats, block), F32)
    loop(0, cubes, add_squares)
    for copy in small[1:]:
        copy.wait()
    sign, bound = label_ref[...].astype(F32), bound_ref[...]

    @pl.when(is_owner)
    def _():
        got0[me] = part0[mine]
        waiting(got0, devices - 1, send_sem.at[0], recv_sem.at[0]).wait_recv()
        margin0 = jnp.sum(got0[...], axis=0)
        side = owned_label[...].astype(F32)
        own0[...] = (owned_bound[...] * side * jnp.maximum(0.0, 1.0 - side * margin0)).astype(BF16)
        all0[mine] = own0[...]
        peers(lambda peer: remote(own0, all0.at[mine], send_sem.at[3], gather_sem.at[cube], peer).start())

    peers(scatter_send(part_d, got_d, 6))
    got_d[me] = part_d[me]
    merge_a(cubes - 2)
    loop(0, cubes - 2, merge_b)
    merge_a(cubes - 1)
    square_total = squares[...]
    column_sq = nt(jnp.ones((8, block), F32), square_total, HIGH)[0:1, :]
    def start_sum(i, total):
        q = low + upward * (cubes - 2 * low - 1 - i) + (1 - upward) * i

        def wait(count):
            view = all0.at[pl.ds(0, count)]
            remote(view, view, send_sem.at[3], gather_sem.at[q], partner).wait_recv()

        own_turn = is_owner & (q == cube)

        @pl.when(own_turn)
        def _():
            wait(3)

        @pl.when(jnp.logical_not(own_turn))
        def _():
            wait(4)

        for j in range(4):
            o = 4 * (q - low) + j
            vector = all0[o].astype(F32)
            for b in range(held):
                row = jnp.concatenate([vector[b * blocks + c:b * blocks + c + 1] for c in range(blocks)], axis=1)
                total = total + nn(spread(row), turned_ref[held * o + b])
        return total

    ascent = lax.fori_loop(0, cubes - 2 * low, start_sum, jnp.zeros((ROWS, feats), F32))[0:1, :]
    scale = column_sq / samples + 1e-06
    stepped = w_start + ascent / (samples * scale)
    thresh = 1.0 / (4.0 * features * scale)
    primal = stepped - jnp.clip(stepped, -thresh, thresh)
    margin_scatter(primal, part1, got1, 1)
    merge_b(cubes - 2)
    merge_c(0)

    def middle_step(i):
        merge_c(i)
        merge_x(i - 1)

    loop(1, cubes - 2, middle_step)
    merge_b(cubes - 1)
    merge_c(cubes - 2)
    merge_x(cubes - 3)
    merge_x(cubes - 2)
    for half in range(2):
        gram_in[cube, half] = merged_c(cubes - 1, half)

    orders, places = [], []
    for b in range(blocks):
        order = (lax.broadcasted_iota(jnp.int32, (block, block), 0) == visit_ref[b:b + 1, :]).astype(F32)
        orders.append(order)
        places.append(order.T.astype(BF16))

    orders_half = [order.astype(BF16) for order in orders]
    twice = [jnp.concatenate([place, place], axis=1) for place in places]

    def upright(row, b):
        piece = row[:, b * block:(b + 1) * block]
        high = piece.astype(BF16).astype(F32)
        both = jnp.broadcast_to(jnp.concatenate([high, piece - high], axis=1), (block, 2 * block))
        return nt(twice[b], both.astype(BF16))

    alpha_zero = bound * frac_ref[...]
    for b in range(blocks):
        sign_c[b] = upright(sign, b)
        bound_c[b] = upright(bound, b)
        alpha_c[b] = upright(alpha_zero, b)
    pick_row = lax.broadcasted_iota(jnp.int32, (block, 2 * block), 0) % GROUP
    pick_lane = lax.broadcasted_iota(jnp.int32, (block, 2 * block), 1) // block
    for r in range(GROUP // 2):
        picks[r] = (pick_row == pick_lane + 2 * r).astype(F32).astype(BF16)

    total_wait(got1, 1).wait_recv()
    total_wait(got_d, 6).wait_recv()
    margin1, diag = jnp.sum(got1[...], axis=0), jnp.sum(got_d[...], axis=0)
    loss = jnp.sum(bound * jnp.square(jnp.maximum(0.0, 1.0 - sign * margin1)), axis=1, keepdims=True)
    penalty = jnp.sum(jnp.abs(primal), axis=1, keepdims=True)
    objective_part = loss / (2.0 * samples) + penalty / (4.0 * features)
    inverse = 0.5 / (diag + 1e-06)
    for b in range(blocks):
        inverse_c[b] = upright(inverse, b)
        margin_c[b] = upright(margin1, b)

    wait_d(0).wait_recv()
    packed = jnp.sum(gram_in[:, 0].astype(F32), axis=0)
    above, below = jnp.where(upper, packed, 0.0), jnp.where(lower, packed, 0.0)
    gap = row_at // GROUP - lane_at // GROUP

    def visited(a, b, piece):
        piece = nn(piece.astype(BF16), orders_half[b]).astype(BF16)
        return nn(places[a], piece)

    for b, piece in enumerate((above + above.T, below + below.T)):
        whole = visited(b, b, piece)
        square[b] = whole
        lagged = [jnp.where(gap == lag, whole, 0.0)[lag * GROUP:] for lag in (1, 2)]
        lagged = jnp.concatenate(lagged, axis=0).astype(BF16)
        for r in range(GROUP // 2):
            spots = nn(lagged, picks[r])
            for c in range(2):
                half = spots[:, c * block:(c + 1) * block]
                table[0, b, 2 * r + c, GROUP:, :] = half[:block - GROUP]
                table[1, b, 2 * r + c, 2 * GROUP:, :] = half[block - GROUP:]
    sub = lax.broadcasted_iota(jnp.int32, (GROUP, block), 0)
    lane = lax.broadcasted_iota(jnp.int32, (GROUP, block), 1)

    def fold(x):
        return x[0:8] + x[8:16]

    def total_of(terms):
        while len(terms) > 1:
            terms = [sum(terms[i:i + 2]) for i in range(0, len(terms), 2)]
        return terms[0]

    def sweep_block(b, offset):
        sets = block // GROUP
        seen, moved, pushes = jnp.zeros((8, block), F32), jnp.zeros((8, block), F32), []
        extra = [[] for _ in range(sets)]
        for s in range(sets):
            at = slice(s * GROUP, (s + 1) * GROUP)
            m = margin_c[b, at]
            if offset is not None:
                m = m + offset[at]
            for term in extra[s]:
                m = m + term
            now, side = alpha_c[b, at], sign_c[b, at]
            fresh = jnp.clip(now + (1.0 - side * m) * inverse_c[b, at], 0.0, bound_c[b, at])
            change = side * (fresh - now)
            alpha_c[b, at] = fresh
            moved = moved + fold(jnp.where(lane == sub + s * GROUP, change, 0.0))
            push = 2.0 * change
            pushes.append(push)
            steps = [jnp.broadcast_to(push[r:r + 1], (GROUP, block)) for r in range(GROUP)]
            if s + 3 < sets:
                seen = seen + fold(push * square[b, at])
                row = jnp.sum(seen, axis=0, keepdims=True)
                spot = jnp.where(lane == sub + (s + 3) * GROUP, row, 0.0)
                extra[s + 3].append(jnp.sum(spot, axis=1, keepdims=True))
            for lag in (2, 1):
                if s + lag < sets:
                    there = slice((s + lag) * GROUP, (s + lag + 1) * GROUP)
                    extra[s + lag].append(
                        total_of([steps[r] * table[lag - 1, b, r, there] for r in range(GROUP)])
                    )
        line = jnp.sum(moved, axis=0, keepdims=True)
        return nt(spread(line), orders_half[b])[0:1, :], pushes

    def passed_on(pushes):
        terms = [fold(push * between_c[s * GROUP:(s + 1) * GROUP]) for s, push in enumerate(pushes)]
        row = jnp.sum(total_of(terms), axis=0, keepdims=True)
        return jnp.sum(jnp.where(even, row, 0.0), axis=1, keepdims=True)

    first, pushes = sweep_block(0, None)
    wait_d(1).wait_recv()
    between_c[...] = visited(0, 1, jnp.sum(gram_in[:, 1].astype(F32), axis=0))
    second, _ = sweep_block(1, passed_on(pushes))
    own1[...] = jnp.concatenate([first, second], axis=0).astype(BF16)
    own_o[...] = jnp.broadcast_to(objective_part, (1, block))
    all_o[me] = own_o[...]
    gather_start(own1, all1, 1 + 3)
    peers(lambda peer: remote(own_o, all_o.at[me], send_sem.at[7], recv_sem.at[4], peer).start())
    update_one = back(all1, 4) * (2.0 / devices)
    margin_scatter(update_one, part2, got2, 2)
    total_wait(all_o, 7).wait_recv()
    out_ref[:, feats + rows:] = jnp.sum(all_o[...], axis=0)
    total_wait(got2, 2).wait_recv()
    margin2 = margin1 + jnp.sum(got2[...], axis=0)
    for b in range(blocks):
        margin_c[b] = upright(margin2, b)
    first, pushes = sweep_block(0, None)
    second, _ = sweep_block(1, passed_on(pushes))
    own2[...] = jnp.concatenate([first, second], axis=0).astype(BF16)
    gather_start(own2, all2, 2 + 3)
    def alpha_out():
        for b in range(blocks):
            spot = jnp.broadcast_to(jnp.sum(jnp.where(even, alpha_c[b], 0.0), axis=0, keepdims=True), (8, block))
            out_ref[:, feats + b * block:feats + (b + 1) * block] = nt(spot, orders[b], HIGH)[0:1, :]

    out_ref[:, :feats] = primal + update_one + back(all2, 5, alpha_out) * (2.0 / devices)

    for phase, ref in ((1, got1), (2, got2), (4, all1), (5, all2), (6, got_d), (7, all_o)):
        total_wait(ref, phase).wait_send()

    @pl.when(is_owner)
    def _():
        waiting(part0, owners - 1, send_sem.at[0], recv_sem.at[0]).wait_send()
        def sent(_):
            remote(own0, all0.at[0], send_sem.at[3], recv_sem.at[0], partner).wait_send()

        loop(0, devices - 1, sent)

    @pl.when(jnp.logical_not(is_owner))
    def _():
        waiting(part0, owners, send_sem.at[0], recv_sem.at[0]).wait_send()

    wait_d(0).wait_send()
    wait_d(1).wait_send()

    def drain(i):
        for j in range(4):
            copy_a(turn(i), j).wait_send()
        for half in range(2):
            for j in range(2):
                copy_b(i, j, half).wait_send()
            copy_c(i, half).wait_send()

    loop(0, cubes, drain)


def split(packed, weights, alpha, objective):
    feats, rows = weights.shape[1], alpha.shape[1]
    weights[...] = packed[:, :feats]
    alpha[...] = packed[:, feats:feats + rows]
    objective[...] = packed[:, feats + rows:feats + rows + 1]


def body(devices, data_t, labels, sample_weight, w_start, alpha_start, visit_order):
    feats = data_t.shape[0]
    rows = alpha_start.shape[0]
    blocks, block = visit_order.shape
    cubes = devices // 8
    owners = cubes // 2 * 4
    span = (devices // owners * blocks, block)
    tiles = [x.reshape(owners, *span) for x in (labels, sample_weight)]
    labels = labels.reshape(devices, 1, rows)
    bound = sample_weight.reshape(devices, 1, rows)

    def grams(count):
        return pltpu.VMEM((count, rows // block, block, block), BF16)

    def semaphores(count):
        return pltpu.SemaphoreType.DMA((count,))

    def vectors(height, length):
        return pltpu.VMEM((devices, height, length), F32)

    vmem = pl.BlockSpec(memory_space=pltpu.VMEM)
    out = pl.pallas_call(
        functools.partial(kernel, devices),
        name="svm_rounds",
        out_shape=jax.ShapeDtypeStruct((1, feats + rows + block), F32),
        in_specs=[pl.BlockSpec(memory_space=pl.ANY)] * 8,
        out_specs=vmem,
        scratch_shapes=[
            pltpu.VMEM((owners, *span), F32), vectors(1, rows), vectors(1, rows), vectors(1, rows),
            pltpu.VMEM((devices, *span), F32), vectors(1, rows), vectors(1, rows), vectors(1, rows),
            pltpu.VMEM(span, BF16), pltpu.VMEM((blocks, block), BF16), pltpu.VMEM((blocks, block), BF16),
            pltpu.VMEM((1, block), F32), pltpu.VMEM((owners, *span), BF16),
            *[pltpu.VMEM((devices, blocks, block), BF16)] * 2, vectors(1, block),
            pltpu.VMEM(data_t.shape, BF16), pltpu.VMEM((devices, rows, feats), BF16), pltpu.VMEM((1, rows), jnp.int32), pltpu.VMEM((1, rows), F32),
            pltpu.VMEM(span, jnp.int32), pltpu.VMEM(span, F32),
            pltpu.VMEM((1, feats), F32), pltpu.VMEM((1, rows), F32), pltpu.VMEM((blocks, block), jnp.int32),
            pltpu.VMEM((feats, block), F32), grams(devices), grams(4 * cubes), grams(2 * cubes), grams(cubes),
            grams(4 * cubes), grams(2 * cubes), grams(cubes), grams(cubes),
            pltpu.VMEM((GROUP // 2, block, 2 * block), BF16), pltpu.VMEM((2, blocks, GROUP, block, block), F32),
            pltpu.VMEM((block, block), F32), *[pltpu.VMEM((blocks, block, block), F32)] * 6,
            semaphores(cubes), semaphores(7), semaphores(8), semaphores(5), semaphores(3 * cubes), semaphores(4 * cubes), semaphores(4 * cubes),
            semaphores(4 * cubes), semaphores(4 * cubes), semaphores(2 * cubes), semaphores(2 * cubes),
            semaphores(2), semaphores(2),
        ],
        compiler_params=pltpu.CompilerParams(
            collective_id=0, has_side_effects=True, vmem_limit_bytes=63 * 1024 * 1024
        ),
    )(data_t, labels, bound, *tiles, w_start[None], alpha_start[None], visit_order)
    weights, alpha, objective = pl.pallas_call(
        split,
        name="split",
        out_shape=(
            jax.ShapeDtypeStruct((1, feats), F32), jax.ShapeDtypeStruct((1, rows), F32), jax.ShapeDtypeStruct((1, 1), F32)
        ),
        in_specs=[vmem],
        out_specs=(vmem, vmem, vmem),
    )(out)
    return weights[0], alpha[0], objective[0, 0]


def solution(mesh):
    placed = (P("shard", None), P(), P(), P("shard"), P("shard"), P("shard", None))
    return jax.shard_map(
        functools.partial(body, mesh.shape["shard"]), mesh=mesh, in_specs=placed,
        out_specs=(P("shard"), P("shard"), P()), check_vma=False,
    )
```

```python
import functools

import jax
import jax.numpy as jnp
from jax import lax
from jax.experimental import pallas as pl
from jax.experimental.pallas import tpu as pltpu
from jax.sharding import PartitionSpec as P

GROUP = 16
ROWS = 16
MESH = pl.DeviceIdType.MESH
F32 = jnp.float32
BF16 = jnp.bfloat16
HIGH = lax.Precision.HIGHEST


def nn(a, b, precision=None):
    return lax.dot_general(a, b, (((1,), (0,)), ((), ())), preferred_element_type=F32, precision=precision)


def nt(a, b, precision=None):
    return lax.dot_general(a, b, (((1,), (1,)), ((), ())), preferred_element_type=F32, precision=precision)


def spread(row):
    return jnp.broadcast_to(row, (ROWS, row.shape[-1])).astype(BF16)


def kernel(
    devices, data_hbm, label_hbm, bound_hbm, label_tiles, bound_tiles, start_hbm, frac_hbm, visit_hbm,
    out_ref,
    part0, part1, part2, part_d, got0, got1, got2, got_d, own0, own1, own2, own_o, all0, all1, all2, all_o,
    data_ref, turned_ref, label_ref, bound_ref, owned_label, owned_bound, start_ref, frac_ref, visit_ref, squares, gram, in_a, in_b, in_c, sum_a, sum_b, sum_c, gram_in,
    picks, table, between_c, square, sign_c, bound_c, inverse_c, alpha_c, margin_c,
    load_sem, small_sem, send_sem, recv_sem, gather_sem, send_a, recv_a, send_b, recv_b, send_c, recv_c, gram_send, gram_recv,
):
    me = lax.axis_index("shard")
    feats, samples = data_hbm.shape
    rows = label_hbm.shape[2]
    blocks, block = visit_hbm.shape
    features = feats * devices
    cubes = devices // 8
    cube = me // 8
    bit0, bit1, bit2 = me % 2, (me // 2) % 2, (me // 4) % 2
    partner = me + 1 - 2 * bit0

    def columns(k):
        return pl.ds(pl.multiple_of(k * rows, rows), rows)

    def loop(first, last, action):
        def step(i, carry):
            action(i)
            return carry

        lax.fori_loop(first, last, step, 0)

    upward = cube // (cubes // 2)
    owners = label_tiles.shape[0]
    held = devices // owners
    low = cubes // 4
    is_owner = (cube >= low) & (cube < cubes - low) & (bit0 == 1)
    mine = jnp.clip(me // 2 - 4 * low, 0, owners - 1)

    def near(i):
        place = upward * (cubes - 2 - i) + (1 - upward) * i
        return place + jnp.where(place >= cube, 1, 0)

    def far(i):
        return near(cubes - 2 - i)

    def mates(action):
        loop(1, 8, lambda i: action(8 * cube + lax.rem(me + i, 8)))

    def cube_of(q, action):
        loop(0, 8, lambda j: action(8 * q + j))

    def peers(action):
        loop(0, cubes - 1, lambda i: cube_of(far(i), action))
        mates(action)

    def remote(source, target, send, recv, peer):
        return pltpu.make_async_remote_copy(
            src_ref=source, dst_ref=target, send_sem=send, recv_sem=recv,
            device_id=(peer,), device_id_type=MESH,
        )

    def total_wait(ref, phase):
        view = ref.at[pl.ds(0, devices - 1)]
        return remote(view, view, send_sem.at[phase], recv_sem.at[phase % 3 if phase < 6 else phase - 3], partner)

    def scatter_send(part, got, phase):
        def send(peer):
            arrived = recv_sem.at[phase if phase < 3 else phase - 3]
            remote(part.at[peer], got.at[me], send_sem.at[phase], arrived, peer).start()

        return send

    def gather_start(own, everyone, phase):
        everyone[me] = own[...]
        spot = (phase - 3) * cubes + cube
        peers(lambda peer: remote(own, everyone.at[me], send_sem.at[phase], gather_sem.at[spot], peer).start())

    def part_of(lhs, part, q):
        for j in range(8):
            k = 8 * q + j
            part[k, 0:1, :] = nn(lhs, data_ref[:, columns(k)])[0:1, :]

    def margin_scatter(row, part, got, phase):
        lhs = spread(row)
        send = scatter_send(part, got, phase)

        def step(i):
            q = far(i)
            part_of(lhs, part, q)
            cube_of(q, send)

        loop(0, cubes - 1, step)
        part_of(lhs, part, cube)
        mates(send)
        got[me] = part[me]

    def back(everyone, phase, meanwhile=None):
        def arrival(q, count):
            view = everyone.at[pl.ds(8 * q, count)]
            spot = (phase - 3) * cubes + q
            remote(view, view, send_sem.at[phase], gather_sem.at[spot], partner).wait_recv()

        def cube_sum(q, total):
            for j in range(8):
                k = 8 * q + j
                vector = everyone[k].astype(F32)
                row = jnp.concatenate([vector[b:b + 1] for b in range(blocks)], axis=1)
                total = total + nn(spread(row), turned_ref[k])
            return total

        def step(i, total):
            q = near(i)
            arrival(q, 8)
            return cube_sum(q, total)

        arrival(cube, 7)
        total = cube_sum(cube, jnp.zeros((ROWS, feats), F32))
        if meanwhile is not None:
            meanwhile()
        return lax.fori_loop(0, cubes - 1, step, total)[0:1, :]

    def load(q):
        view = pl.ds(pl.multiple_of(8 * q * rows, rows), 8 * rows)
        return pltpu.make_async_copy(data_hbm.at[:, view], data_ref.at[:, view], load_sem.at[q])

    small = [
        pltpu.make_async_copy(source, target, small_sem.at[i])
        for i, (source, target) in enumerate((
            (start_hbm, start_ref), (label_hbm.at[me], label_ref), (bound_hbm.at[me], bound_ref),
            (frac_hbm, frac_ref), (visit_hbm, visit_ref),
            (label_tiles.at[mine], owned_label), (bound_tiles.at[mine], owned_bound),
        ))
    ]
    small[0].start()
    loop(0, cubes - 1, lambda i: load(far(i)).start())
    load(cube).start()
    for copy in small[1:]:
        copy.start()
    barrier = pltpu.get_barrier_semaphore()
    peers(lambda peer: pl.semaphore_signal(barrier, inc=1, device_id=(peer,), device_id_type=MESH))

    row_at = lax.broadcasted_iota(jnp.int32, (block, block), 0)
    lane_at = lax.broadcasted_iota(jnp.int32, (block, block), 1)
    upper, lower, even = row_at < lane_at, row_at > lane_at, row_at == lane_at

    def gram_of(k):
        tile = data_ref[:, columns(k)]
        first, second = tile[:, :block], tile[:, block:]
        turned = tile.T
        turned_ref[k] = turned
        top, low = nn(turned[:block], tile), nn(turned[block:], second)
        gram[k, 0] = jnp.where(upper, top[:, :block], low).astype(BF16)
        gram[k, 1] = top[:, block:].astype(BF16)
        part_d[k, 0:1, :block] = jnp.sum(jnp.where(even, top[:, :block], 0.0), axis=0, keepdims=True)
        part_d[k, 0:1, block:] = jnp.sum(jnp.where(even, low, 0.0), axis=0, keepdims=True)

    def halving(source, target, index, sends, recvs, peer):
        return pltpu.make_async_remote_copy(
            src_ref=source, dst_ref=target, send_sem=sends.at[0],
            recv_sem=recvs.at[index], device_id=(peer,), device_id_type=MESH,
        )

    def copy_a(q, j):
        return halving(gram.at[8 * q + 2 * j + 1 - bit0], in_a.at[4 * q + j], q, send_a, recv_a, partner)

    orders_of = ((bit1, 1, bit2, 2), (bit2, 2, bit1, 1))

    def copy_b(i, t, half):
        q = turn(i)
        bit, weight, _, other = orders_of[half]
        return halving(
            sum_a.at[4 * q + weight * (1 - bit) + other * t, half], in_b.at[2 * q + t, half],
            q, send_b, recv_b, me + 2 * weight * (1 - 2 * bit),
        )

    def copy_c(i, half):
        q = turn(i)
        _, _, bit, weight = orders_of[half]
        return halving(
            sum_b.at[2 * q + 1 - bit, half], in_c.at[q, half],
            q, send_c, recv_c, me + 2 * weight * (1 - 2 * bit),
        )

    def copy_d(q, half):
        return pltpu.make_async_remote_copy(
            src_ref=sum_c.at[q, half], dst_ref=gram_in.at[cube, half], send_sem=gram_send.at[half],
            recv_sem=gram_recv.at[half], device_id=(me + 8 * (q - cube),), device_id_type=MESH,
        )

    def wait_d(half):
        view = gram_in.at[pl.ds(0, cubes - 1), half]
        return pltpu.make_async_remote_copy(
            src_ref=view, dst_ref=view, send_sem=gram_send.at[half], recv_sem=gram_recv.at[half],
            device_id=(partner,), device_id_type=MESH,
        )

    def added(x, y):
        return (x.astype(F32) + y.astype(F32)).astype(BF16)

    def turn(i):
        return jnp.where(i == cubes - 1, cube, far(jnp.minimum(i, cubes - 2)))

    def merge_a(i):
        q = turn(i)
        stage_wait(in_a, 4 * q, 4, q, send_a, recv_a).wait_recv()
        for j in range(4):
            sum_a[4 * q + j] = added(gram[8 * q + 2 * j + bit0], in_a[4 * q + j])
        for half in range(2):
            for t in (1 - orders_of[half][2], orders_of[half][2]):
                copy_b(i, t, half).start()

    def merge_b(i):
        q = turn(i)
        stage_wait(in_b, 2 * q, 2, q, send_b, recv_b).wait_recv()
        for half in range(2):
            bit, weight, last, other = orders_of[half]
            for t in (1 - last, last):
                sum_b[2 * q + t, half] = added(
                    sum_a[4 * q + weight * bit + other * t, half], in_b[2 * q + t, half]
                )
            copy_c(i, half).start()

    def merged_c(i, half):
        q = turn(i)
        return added(sum_b[2 * q + orders_of[half][2], half], in_c[q, half])

    def merge_c(i):
        q = turn(i)
        stage_wait(in_c, q, 1, q, send_c, recv_c).wait_recv()
        for half in range(2):
            sum_c[q, half] = merged_c(i, half)
        copy_d(q, 0).start()

    def merge_x(i):
        copy_d(turn(i), 1).start()

    def stage_wait(ref, first, count, index, sends, recvs):
        view = ref.at[pl.ds(first, count)]
        return halving(view, view, index, sends, recvs, partner)

    def start_a(i):
        for j in range(4):
            copy_a(turn(i), j).start()

    def gram_part(i, side):
        for j in range(4):
            gram_of(8 * turn(i) + 2 * j + side)

    def gram_step(i):
        gram_part(i, 1 - bit0)
        start_a(i)
        gram_part(i, bit0)

    small[0].wait()
    w_start = start_ref[...]
    start_rows = spread(w_start)

    def add_squares(q):
        for r in range(0, feats, 32):
            total = squares[r:r + 32, :]
            for j in range(8 * blocks):
                at = pl.ds(pl.multiple_of(8 * q * rows + j * block, block), block)
                piece = data_ref[r:r + 32, at].astype(F32)
                total = total + piece * piece
            squares[r:r + 32, :] = total

    def first_part(q):
        load(q).wait()
        for j in range(8):
            row = nn(start_rows, data_ref[:, columns(8 * q + j)])
            for b in range(blocks):
                at = j % held * blocks + b
                part0[8 // held * q + j // held, at:at + 1, :] = row[0:1, b * block:(b + 1) * block]

    def each_owner(action):
        def step(i):
            o = upward * i + (1 - upward) * (owners - 1 - i)
            peer = 8 * low + 2 * o + 1

            @pl.when(peer != me)
            def _():
                action(o, peer)

        loop(0, owners, step)

    def owned(ref, count):
        return ref.at[pl.ds(0, count)]

    def waiting(ref, count, send, recv):
        view = owned(ref, count)
        return remote(view, view, send, recv, partner)

    first_part(far(0))
    gram_part(0, 1 - bit0)
    gram_part(0, bit0)
    loop(1, cubes - 1, lambda i: first_part(far(i)))
    first_part(cube)
    pl.semaphore_wait(barrier, devices - 1)
    each_owner(lambda o, peer: remote(part0.at[o], got0.at[me], send_sem.at[0], recv_sem.at[0], peer).start())
    start_a(0)

    def early_step(i):
        gram_step(i)
        merge_a(i - 1)

    loop(1, cubes - 1, early_step)
    gram_step(cubes - 1)
    squares[...] = jnp.zeros((feats, block), F32)
    loop(0, cubes, add_squares)
    for copy in small[1:]:
        copy.wait()
    sign, bound = label_ref[...].astype(F32), bound_ref[...]

    @pl.when(is_owner)
    def _():
        got0[me] = part0[mine]
        waiting(got0, devices - 1, send_sem.at[0], recv_sem.at[0]).wait_recv()
        margin0 = jnp.sum(got0[...], axis=0)
        side = owned_label[...].astype(F32)
        own0[...] = (owned_bound[...] * side * jnp.maximum(0.0, 1.0 - side * margin0)).astype(BF16)
        all0[mine] = own0[...]
        peers(lambda peer: remote(own0, all0.at[mine], send_sem.at[3], gather_sem.at[cube], peer).start())

    peers(scatter_send(part_d, got_d, 6))
    got_d[me] = part_d[me]
    merge_a(cubes - 2)
    loop(0, cubes - 2, merge_b)
    merge_a(cubes - 1)
    square_total = squares[...]
    column_sq = nt(jnp.ones((8, block), F32), square_total, HIGH)[0:1, :]
    def start_sum(i, total):
        q = low + upward * (cubes - 2 * low - 1 - i) + (1 - upward) * i

        def wait(count):
            view = all0.at[pl.ds(0, count)]
            remote(view, view, send_sem.at[3], gather_sem.at[q], partner).wait_recv()

        own_turn = is_owner & (q == cube)

        @pl.when(own_turn)
        def _():
            wait(3)

        @pl.when(jnp.logical_not(own_turn))
        def _():
            wait(4)

        for j in range(4):
            o = 4 * (q - low) + j
            vector = all0[o].astype(F32)
            for b in range(held):
                row = jnp.concatenate([vector[b * blocks + c:b * blocks + c + 1] for c in range(blocks)], axis=1)
                total = total + nn(spread(row), turned_ref[held * o + b])
        return total

    ascent = lax.fori_loop(0, cubes - 2 * low, start_sum, jnp.zeros((ROWS, feats), F32))[0:1, :]
    scale = column_sq / samples + 1e-06
    stepped = w_start + ascent / (samples * scale)
    thresh = 1.0 / (4.0 * features * scale)
    primal = stepped - jnp.clip(stepped, -thresh, thresh)
    margin_scatter(primal, part1, got1, 1)
    merge_b(cubes - 2)
    merge_c(0)

    def middle_step(i):
        merge_c(i)
        merge_x(i - 1)

    loop(1, cubes - 2, middle_step)
    merge_b(cubes - 1)
    merge_c(cubes - 2)
    merge_x(cubes - 3)
    merge_x(cubes - 2)
    orders, places = [], []
    for b in range(blocks):
        order = (lax.broadcasted_iota(jnp.int32, (block, block), 0) == visit_ref[b:b + 1, :]).astype(F32)
        orders.append(order)
        places.append(order.T.astype(BF16))

    orders_half = [order.astype(BF16) for order in orders]
    twice = [jnp.concatenate([place, place], axis=1) for place in places]

    def upright(row, b):
        piece = row[:, b * block:(b + 1) * block]
        high = piece.astype(BF16).astype(F32)
        both = jnp.broadcast_to(jnp.concatenate([high, piece - high], axis=1), (block, 2 * block))
        return nt(twice[b], both.astype(BF16))

    alpha_zero = bound * frac_ref[...]
    for b in range(blocks):
        sign_c[b] = upright(sign, b)
        bound_c[b] = upright(bound, b)
        alpha_c[b] = upright(alpha_zero, b)
    pick_row = lax.broadcasted_iota(jnp.int32, (block, 2 * block), 0) % GROUP
    pick_lane = lax.broadcasted_iota(jnp.int32, (block, 2 * block), 1) // block
    for r in range(GROUP // 2):
        picks[r] = (pick_row == pick_lane + 2 * r).astype(F32).astype(BF16)

    total_wait(got1, 1).wait_recv()
    total_wait(got_d, 6).wait_recv()
    margin1, diag = jnp.sum(got1[...], axis=0), jnp.sum(got_d[...], axis=0)
    loss = jnp.sum(bound * jnp.square(jnp.maximum(0.0, 1.0 - sign * margin1)), axis=1, keepdims=True)
    penalty = jnp.sum(jnp.abs(primal), axis=1, keepdims=True)
    objective_part = loss / (2.0 * samples) + penalty / (4.0 * features)
    inverse = 0.5 / (diag + 1e-06)
    for b in range(blocks):
        inverse_c[b] = upright(inverse, b)
        margin_c[b] = upright(margin1, b)

    stage_wait(in_c, cube, 1, cube, send_c, recv_c).wait_recv()
    for half in range(2):
        gram_in[cube, half] = merged_c(cubes - 1, half)

    wait_d(0).wait_recv()
    packed = jnp.sum(gram_in[:, 0].astype(F32), axis=0)
    above, below = jnp.where(upper, packed, 0.0), jnp.where(lower, packed, 0.0)
    gap = row_at // GROUP - lane_at // GROUP

    def visited(a, b, piece):
        piece = nn(piece.astype(BF16), orders_half[b]).astype(BF16)
        return nn(places[a], piece)

    for b, piece in enumerate((above + above.T, below + below.T)):
        whole = visited(b, b, piece)
        square[b] = whole
        lagged = [jnp.where(gap == lag, whole, 0.0)[lag * GROUP:] for lag in (1, 2)]
        lagged = jnp.concatenate(lagged, axis=0).astype(BF16)
        for r in range(GROUP // 2):
            spots = nn(lagged, picks[r])
            for c in range(2):
                half = spots[:, c * block:(c + 1) * block]
                table[0, b, 2 * r + c, GROUP:, :] = half[:block - GROUP]
                table[1, b, 2 * r + c, 2 * GROUP:, :] = half[block - GROUP:]
    sub = lax.broadcasted_iota(jnp.int32, (GROUP, block), 0)
    lane = lax.broadcasted_iota(jnp.int32, (GROUP, block), 1)

    def fold(x):
        return x[0:8] + x[8:16]

    def total_of(terms):
        while len(terms) > 1:
            terms = [sum(terms[i:i + 2]) for i in range(0, len(terms), 2)]
        return terms[0]

    def sweep_block(b, offset):
        sets = block // GROUP
        seen, moved, pushes = jnp.zeros((8, block), F32), jnp.zeros((8, block), F32), []
        extra = [[] for _ in range(sets)]
        for s in range(sets):
            at = slice(s * GROUP, (s + 1) * GROUP)
            m = margin_c[b, at]
            if offset is not None:
                m = m + offset[at]
            for term in extra[s]:
                m = m + term
            now, side = alpha_c[b, at], sign_c[b, at]
            fresh = jnp.clip(now + (1.0 - side * m) * inverse_c[b, at], 0.0, bound_c[b, at])
            change = side * (fresh - now)
            alpha_c[b, at] = fresh
            moved = moved + fold(jnp.where(lane == sub + s * GROUP, change, 0.0))
            push = 2.0 * change
            pushes.append(push)
            steps = [jnp.broadcast_to(push[r:r + 1], (GROUP, block)) for r in range(GROUP)]
            if s + 3 < sets:
                seen = seen + fold(push * square[b, at])
                row = jnp.sum(seen, axis=0, keepdims=True)
                spot = jnp.where(lane == sub + (s + 3) * GROUP, row, 0.0)
                extra[s + 3].append(jnp.sum(spot, axis=1, keepdims=True))
            for lag in (2, 1):
                if s + lag < sets:
                    there = slice((s + lag) * GROUP, (s + lag + 1) * GROUP)
                    extra[s + lag].append(
                        total_of([steps[r] * table[lag - 1, b, r, there] for r in range(GROUP)])
                    )
        line = jnp.sum(moved, axis=0, keepdims=True)
        return nt(spread(line), orders_half[b])[0:1, :], pushes

    def passed_on(pushes):
        terms = [fold(push * between_c[s * GROUP:(s + 1) * GROUP]) for s, push in enumerate(pushes)]
        row = jnp.sum(total_of(terms), axis=0, keepdims=True)
        return jnp.sum(jnp.where(even, row, 0.0), axis=1, keepdims=True)

    first, pushes = sweep_block(0, None)
    wait_d(1).wait_recv()
    between_c[...] = visited(0, 1, jnp.sum(gram_in[:, 1].astype(F32), axis=0))
    second, _ = sweep_block(1, passed_on(pushes))
    own1[...] = jnp.concatenate([first, second], axis=0).astype(BF16)
    own_o[...] = jnp.broadcast_to(objective_part, (1, block))
    all_o[me] = own_o[...]
    gather_start(own1, all1, 1 + 3)
    peers(lambda peer: remote(own_o, all_o.at[me], send_sem.at[7], recv_sem.at[4], peer).start())
    update_one = back(all1, 4) * (2.0 / devices)
    margin_scatter(update_one, part2, got2, 2)
    total_wait(all_o, 7).wait_recv()
    out_ref[:, feats + rows:] = jnp.sum(all_o[...], axis=0)
    total_wait(got2, 2).wait_recv()
    margin2 = margin1 + jnp.sum(got2[...], axis=0)
    for b in range(blocks):
        margin_c[b] = upright(margin2, b)
    first, pushes = sweep_block(0, None)
    second, _ = sweep_block(1, passed_on(pushes))
    own2[...] = jnp.concatenate([first, second], axis=0).astype(BF16)
    gather_start(own2, all2, 2 + 3)
    def alpha_out():
        for b in range(blocks):
            spot = jnp.broadcast_to(jnp.sum(jnp.where(even, alpha_c[b], 0.0), axis=0, keepdims=True), (8, block))
            out_ref[:, feats + b * block:feats + (b + 1) * block] = nt(spot, orders[b], HIGH)[0:1, :]

    out_ref[:, :feats] = primal + update_one + back(all2, 5, alpha_out) * (2.0 / devices)

    for phase, ref in ((1, got1), (2, got2), (4, all1), (5, all2), (6, got_d), (7, all_o)):
        total_wait(ref, phase).wait_send()

    @pl.when(is_owner)
    def _():
        waiting(part0, owners - 1, send_sem.at[0], recv_sem.at[0]).wait_send()
        def sent(_):
            remote(own0, all0.at[0], send_sem.at[3], recv_sem.at[0], partner).wait_send()

        loop(0, devices - 1, sent)

    @pl.when(jnp.logical_not(is_owner))
    def _():
        waiting(part0, owners, send_sem.at[0], recv_sem.at[0]).wait_send()

    wait_d(0).wait_send()
    wait_d(1).wait_send()

    stage_wait(in_a, 0, 4 * cubes, 0, send_a, recv_a).wait_send()
    stage_wait(in_b, 0, 2 * cubes, 0, send_b, recv_b).wait_send()
    stage_wait(in_c, 0, cubes, 0, send_c, recv_c).wait_send()


def split(packed, weights, alpha, objective):
    feats, rows = weights.shape[1], alpha.shape[1]
    weights[...] = packed[:, :feats]
    alpha[...] = packed[:, feats:feats + rows]
    objective[...] = packed[:, feats + rows:feats + rows + 1]


def body(devices, data_t, labels, sample_weight, w_start, alpha_start, visit_order):
    feats = data_t.shape[0]
    rows = alpha_start.shape[0]
    blocks, block = visit_order.shape
    cubes = devices // 8
    owners = cubes // 2 * 4
    span = (devices // owners * blocks, block)
    tiles = [x.reshape(owners, *span) for x in (labels, sample_weight)]
    labels = labels.reshape(devices, 1, rows)
    bound = sample_weight.reshape(devices, 1, rows)

    def grams(count):
        return pltpu.VMEM((count, rows // block, block, block), BF16)

    def semaphores(count):
        return pltpu.SemaphoreType.DMA((count,))

    def vectors(height, length):
        return pltpu.VMEM((devices, height, length), F32)

    vmem = pl.BlockSpec(memory_space=pltpu.VMEM)
    out = pl.pallas_call(
        functools.partial(kernel, devices),
        name="svm_rounds",
        out_shape=jax.ShapeDtypeStruct((1, feats + rows + block), F32),
        in_specs=[pl.BlockSpec(memory_space=pltpu.HBM)] * 8,
        out_specs=vmem,
        scratch_shapes=[
            pltpu.VMEM((owners, *span), F32), vectors(1, rows), vectors(1, rows), vectors(1, rows),
            pltpu.VMEM((devices, *span), F32), vectors(1, rows), vectors(1, rows), vectors(1, rows),
            pltpu.VMEM(span, BF16), pltpu.VMEM((blocks, block), BF16), pltpu.VMEM((blocks, block), BF16),
            pltpu.VMEM((1, block), F32), pltpu.VMEM((owners, *span), BF16),
            *[pltpu.VMEM((devices, blocks, block), BF16)] * 2, vectors(1, block),
            pltpu.VMEM(data_t.shape, BF16), pltpu.VMEM((devices, rows, feats), BF16), pltpu.VMEM((1, rows), jnp.int32), pltpu.VMEM((1, rows), F32),
            pltpu.VMEM(span, jnp.int32), pltpu.VMEM(span, F32),
            pltpu.VMEM((1, feats), F32), pltpu.VMEM((1, rows), F32), pltpu.VMEM((blocks, block), jnp.int32),
            pltpu.VMEM((feats, block), F32), grams(devices), grams(4 * cubes), grams(2 * cubes), grams(cubes),
            grams(4 * cubes), grams(2 * cubes), grams(cubes), grams(cubes),
            pltpu.VMEM((GROUP // 2, block, 2 * block), BF16), pltpu.VMEM((2, blocks, GROUP, block, block), F32),
            pltpu.VMEM((block, block), F32), *[pltpu.VMEM((blocks, block, block), F32)] * 6,
            semaphores(cubes), semaphores(7), semaphores(8), semaphores(5), semaphores(3 * cubes),
            semaphores(1), semaphores(cubes), semaphores(1), semaphores(cubes), semaphores(1), semaphores(cubes),
            semaphores(2), semaphores(2),
        ],
        compiler_params=pltpu.CompilerParams(
            collective_id=0, has_side_effects=True, vmem_limit_bytes=48 * 1024 * 1024
        ),
    )(*[
        pltpu.with_memory_space_constraint(x, pltpu.HBM)
        for x in (data_t, labels, bound, *tiles, w_start[None], alpha_start[None], visit_order)
    ])
    weights, alpha, objective = pl.pallas_call(
        split,
        name="split",
        out_shape=(
            jax.ShapeDtypeStruct((1, feats), F32), jax.ShapeDtypeStruct((1, rows), F32), jax.ShapeDtypeStruct((1, 1), F32)
        ),
        in_specs=[vmem],
        out_specs=(vmem, vmem, vmem),
        compiler_params=pltpu.CompilerParams(vmem_limit_bytes=1024 * 1024),
    )(out)
    return weights[0], alpha[0], objective[0, 0]


def solution(mesh):
    placed = (P("shard", None), P(), P(), P("shard"), P("shard"), P("shard", None))
    return jax.shard_map(
        functools.partial(body, mesh.shape["shard"]), mesh=mesh, in_specs=placed,
        out_specs=(P("shard"), P("shard"), P()), check_vma=False,
    )
```

```python
import functools

import jax
import jax.numpy as jnp
from jax import lax
from jax.experimental import pallas as pl
from jax.experimental.pallas import tpu as pltpu
from jax.sharding import PartitionSpec as P

GROUP = 16
ROWS = 16
MESH = pl.DeviceIdType.MESH
F32 = jnp.float32
BF16 = jnp.bfloat16
HIGH = lax.Precision.HIGHEST


def nn(a, b, precision=None):
    return lax.dot_general(a, b, (((1,), (0,)), ((), ())), preferred_element_type=F32, precision=precision)


def nt(a, b, precision=None):
    return lax.dot_general(a, b, (((1,), (1,)), ((), ())), preferred_element_type=F32, precision=precision)


def spread(row):
    return jnp.broadcast_to(row, (ROWS, row.shape[-1])).astype(BF16)


def kernel(
    devices, data_hbm, label_hbm, bound_hbm, label_tiles, bound_tiles, start_hbm, frac_hbm, visit_hbm,
    out_ref,
    part0, part1, part2, part_d, got0, got1, got2, got_d, own0, own1, own2, own_o, all0, all1, all2, all_o,
    data_ref, turned_ref, label_ref, bound_ref, owned_label, owned_bound, start_ref, frac_ref, visit_ref, squares, gram, in_a, in_b, in_c, sum_a, sum_b, sum_c, gram_in,
    picks, table, between_c, square, sign_c, bound_c, inverse_c, alpha_c, margin_c,
    load_sem, small_sem, send_sem, recv_sem, gather_sem, send_a, recv_a, send_b, recv_b, send_c, recv_c, gram_send, gram_recv,
):
    me = lax.axis_index("shard")
    feats, samples = data_hbm.shape
    rows = label_hbm.shape[2]
    blocks, block = visit_hbm.shape
    features = feats * devices
    cubes = devices // 8
    cube = me // 8
    bit0, bit1, bit2 = me % 2, (me // 2) % 2, (me // 4) % 2
    partner = me + 1 - 2 * bit0

    def columns(k):
        return pl.ds(pl.multiple_of(k * rows, rows), rows)

    def loop(first, last, action):
        def step(i, carry):
            action(i)
            return carry

        lax.fori_loop(first, last, step, 0)

    upward = cube // (cubes // 2)
    owners = label_tiles.shape[0]
    held = devices // owners
    low = cubes // 4
    is_owner = (cube >= low) & (cube < cubes - low) & (bit0 == 1)
    mine = jnp.clip(me // 2 - 4 * low, 0, owners - 1)

    def near(i):
        place = upward * (cubes - 2 - i) + (1 - upward) * i
        return place + jnp.where(place >= cube, 1, 0)

    def far(i):
        return near(cubes - 2 - i)

    def mates(action):
        loop(1, 8, lambda i: action(8 * cube + lax.rem(me + i, 8)))

    def cube_of(q, action):
        loop(0, 8, lambda j: action(8 * q + j))

    def peers(action):
        loop(0, cubes - 1, lambda i: cube_of(far(i), action))
        mates(action)

    def remote(source, target, send, recv, peer):
        return pltpu.make_async_remote_copy(
            src_ref=source, dst_ref=target, send_sem=send, recv_sem=recv,
            device_id=(peer,), device_id_type=MESH,
        )

    def total_wait(ref, phase):
        view = ref.at[pl.ds(0, devices - 1)]
        return remote(view, view, send_sem.at[phase], recv_sem.at[phase % 3 if phase < 6 else phase - 3], partner)

    def scatter_send(part, got, phase):
        def send(peer):
            arrived = recv_sem.at[phase if phase < 3 else phase - 3]
            remote(part.at[peer], got.at[me], send_sem.at[phase], arrived, peer).start()

        return send

    def gather_start(own, everyone, phase):
        everyone[me] = own[...]
        spot = (phase - 3) * cubes - 2 * low + cube
        peers(lambda peer: remote(own, everyone.at[me], send_sem.at[phase], gather_sem.at[spot], peer).start())

    def part_of(lhs, part, q):
        for j in range(8):
            k = 8 * q + j
            part[k, 0:1, :] = nn(lhs, data_ref[:, columns(k)])[0:1, :]

    def margin_scatter(row, part, got, phase):
        lhs = spread(row)
        send = scatter_send(part, got, phase)

        def step(i):
            q = far(i)
            part_of(lhs, part, q)
            cube_of(q, send)

        loop(0, cubes - 1, step)
        part_of(lhs, part, cube)
        mates(send)
        got[me] = part[me]

    def back(everyone, phase, meanwhile=None):
        def arrival(q, count):
            view = everyone.at[pl.ds(8 * q, count)]
            spot = (phase - 3) * cubes - 2 * low + q
            remote(view, view, send_sem.at[phase], gather_sem.at[spot], partner).wait_recv()

        def cube_sum(q, total):
            for j in range(8):
                k = 8 * q + j
                vector = everyone[k].astype(F32)
                row = jnp.concatenate([vector[b:b + 1] for b in range(blocks)], axis=1)
                total = total + nn(spread(row), turned_ref[k])
            return total

        def step(i, total):
            q = near(i)
            arrival(q, 8)
            return cube_sum(q, total)

        arrival(cube, 7)
        total = cube_sum(cube, jnp.zeros((ROWS, feats), F32))
        if meanwhile is not None:
            meanwhile()
        return lax.fori_loop(0, cubes - 1, step, total)[0:1, :]

    def load(q):
        view = pl.ds(pl.multiple_of(8 * q * rows, rows), 8 * rows)
        return pltpu.make_async_copy(data_hbm.at[:, view], data_ref.at[:, view], load_sem.at[q])

    small = [
        pltpu.make_async_copy(source, target, small_sem.at[i])
        for i, (source, target) in enumerate((
            (start_hbm, start_ref), (label_hbm.at[me], label_ref), (bound_hbm.at[me], bound_ref),
            (frac_hbm, frac_ref), (visit_hbm, visit_ref),
            (label_tiles.at[mine], owned_label), (bound_tiles.at[mine], owned_bound),
        ))
    ]
    small[0].start()
    loop(0, cubes - 1, lambda i: load(far(i)).start())
    load(cube).start()
    for copy in small[1:]:
        copy.start()
    barrier = pltpu.get_barrier_semaphore()
    peers(lambda peer: pl.semaphore_signal(barrier, inc=1, device_id=(peer,), device_id_type=MESH))

    row_at = lax.broadcasted_iota(jnp.int32, (block, block), 0)
    lane_at = lax.broadcasted_iota(jnp.int32, (block, block), 1)
    upper, lower, even = row_at < lane_at, row_at > lane_at, row_at == lane_at

    def gram_of(k):
        tile = data_ref[:, columns(k)]
        first, second = tile[:, :block], tile[:, block:]
        turned = tile.T
        turned_ref[k] = turned
        top, low = nn(turned[:block], tile), nn(turned[block:], second)
        gram[k, 0] = jnp.where(upper, top[:, :block], low).astype(BF16)
        gram[k, 1] = top[:, block:].astype(BF16)
        part_d[k, 0:1, :block] = jnp.sum(jnp.where(even, top[:, :block], 0.0), axis=0, keepdims=True)
        part_d[k, 0:1, block:] = jnp.sum(jnp.where(even, low, 0.0), axis=0, keepdims=True)

    def halving(source, target, index, sends, recvs, peer):
        return pltpu.make_async_remote_copy(
            src_ref=source, dst_ref=target, send_sem=sends.at[0],
            recv_sem=recvs.at[index], device_id=(peer,), device_id_type=MESH,
        )

    def copy_a(q, j):
        return halving(gram.at[8 * q + 2 * j + 1 - bit0], in_a.at[4 * q + j], q, send_a, recv_a, partner)

    orders_of = ((bit1, 1, bit2, 2), (bit2, 2, bit1, 1))

    def copy_b(i, t, half):
        q = turn(i)
        bit, weight, _, other = orders_of[half]
        return halving(
            sum_a.at[4 * q + weight * (1 - bit) + other * t, half], in_b.at[2 * q + t, half],
            q, send_b, recv_b, me + 2 * weight * (1 - 2 * bit),
        )

    def copy_c(i, half):
        q = turn(i)
        _, _, bit, weight = orders_of[half]
        return halving(
            sum_b.at[2 * q + 1 - bit, half], in_c.at[q, half],
            q, send_c, recv_c, me + 2 * weight * (1 - 2 * bit),
        )

    def copy_d(q, half):
        return pltpu.make_async_remote_copy(
            src_ref=sum_c.at[q, half], dst_ref=gram_in.at[cube, half], send_sem=gram_send.at[0],
            recv_sem=gram_recv.at[half], device_id=(me + 8 * (q - cube),), device_id_type=MESH,
        )

    def wait_d(half):
        view = gram_in.at[pl.ds(0, cubes - 1), half]
        return pltpu.make_async_remote_copy(
            src_ref=view, dst_ref=view, send_sem=gram_send.at[0], recv_sem=gram_recv.at[half],
            device_id=(partner,), device_id_type=MESH,
        )

    def added(x, y):
        return (x.astype(F32) + y.astype(F32)).astype(BF16)

    def turn(i):
        return jnp.where(i == cubes - 1, cube, far(jnp.minimum(i, cubes - 2)))

    def merge_a(i):
        q = turn(i)
        stage_wait(in_a, 4 * q, 4, q, send_a, recv_a).wait_recv()
        for j in range(4):
            sum_a[4 * q + j] = added(gram[8 * q + 2 * j + bit0], in_a[4 * q + j])
        for half in range(2):
            for t in (1 - orders_of[half][2], orders_of[half][2]):
                copy_b(i, t, half).start()

    def merge_b(i):
        q = turn(i)
        stage_wait(in_b, 2 * q, 2, q, send_b, recv_b).wait_recv()
        for half in range(2):
            bit, weight, last, other = orders_of[half]
            for t in (1 - last, last):
                sum_b[2 * q + t, half] = added(
                    sum_a[4 * q + weight * bit + other * t, half], in_b[2 * q + t, half]
                )
            copy_c(i, half).start()

    def merged_c(i, half):
        q = turn(i)
        return added(sum_b[2 * q + orders_of[half][2], half], in_c[q, half])

    def merge_c(i):
        q = turn(i)
        stage_wait(in_c, q, 1, q, send_c, recv_c).wait_recv()
        for half in range(2):
            sum_c[q, half] = merged_c(i, half)
        copy_d(q, 0).start()

    def merge_x(i):
        copy_d(turn(i), 1).start()

    def stage_wait(ref, first, count, index, sends, recvs):
        view = ref.at[pl.ds(first, count)]
        return halving(view, view, index, sends, recvs, partner)

    def start_a(i):
        for j in range(4):
            copy_a(turn(i), j).start()

    def gram_part(i, side):
        for j in range(4):
            gram_of(8 * turn(i) + 2 * j + side)

    def gram_step(i):
        gram_part(i, 1 - bit0)
        start_a(i)
        gram_part(i, bit0)

    small[0].wait()
    w_start = start_ref[...]
    start_rows = spread(w_start)

    def add_squares(q):
        for r in range(0, feats, 32):
            total = squares[r:r + 32, :]
            for j in range(8 * blocks):
                at = pl.ds(pl.multiple_of(8 * q * rows + j * block, block), block)
                piece = data_ref[r:r + 32, at].astype(F32)
                total = total + piece * piece
            squares[r:r + 32, :] = total

    def first_part(q):
        load(q).wait()
        for j in range(8):
            row = nn(start_rows, data_ref[:, columns(8 * q + j)])
            for b in range(blocks):
                at = j % held * blocks + b
                part0[8 // held * q + j // held, at:at + 1, :] = row[0:1, b * block:(b + 1) * block]

    def each_owner(action):
        def step(i):
            o = upward * i + (1 - upward) * (owners - 1 - i)
            peer = 8 * low + 2 * o + 1

            @pl.when(peer != me)
            def _():
                action(o, peer)

        loop(0, owners, step)

    def owned(ref, count):
        return ref.at[pl.ds(0, count)]

    def waiting(ref, count, send, recv):
        view = owned(ref, count)
        return remote(view, view, send, recv, partner)

    first_part(far(0))
    gram_part(0, 1 - bit0)
    gram_part(0, bit0)
    loop(1, cubes - 1, lambda i: first_part(far(i)))
    first_part(cube)
    pl.semaphore_wait(barrier, devices - 1)
    each_owner(lambda o, peer: remote(part0.at[o], got0.at[me], send_sem.at[0], recv_sem.at[0], peer).start())
    start_a(0)

    def early_step(i):
        gram_step(i)
        merge_a(i - 1)

    loop(1, cubes - 1, early_step)
    gram_step(cubes - 1)
    squares[...] = jnp.zeros((feats, block), F32)
    loop(0, cubes, add_squares)
    for copy in small[1:]:
        copy.wait()
    sign, bound = label_ref[...].astype(F32), bound_ref[...]

    @pl.when(is_owner)
    def _():
        got0[me] = part0[mine]
        waiting(got0, devices - 1, send_sem.at[0], recv_sem.at[0]).wait_recv()
        margin0 = jnp.sum(got0[...], axis=0)
        side = owned_label[...].astype(F32)
        own0[...] = (owned_bound[...] * side * jnp.maximum(0.0, 1.0 - side * margin0)).astype(BF16)
        all0[mine] = own0[...]
        peers(lambda peer: remote(own0, all0.at[mine], send_sem.at[3], gather_sem.at[cube - low], peer).start())

    peers(scatter_send(part_d, got_d, 6))
    got_d[me] = part_d[me]
    merge_a(cubes - 2)
    loop(0, cubes - 2, merge_b)
    merge_a(cubes - 1)
    square_total = squares[...]
    column_sq = nt(jnp.ones((8, block), F32), square_total, HIGH)[0:1, :]
    def start_sum(i, total):
        q = low + upward * (cubes - 2 * low - 1 - i) + (1 - upward) * i

        def wait(count):
            view = all0.at[pl.ds(0, count)]
            remote(view, view, send_sem.at[3], gather_sem.at[q - low], partner).wait_recv()

        own_turn = is_owner & (q == cube)

        @pl.when(own_turn)
        def _():
            wait(3)

        @pl.when(jnp.logical_not(own_turn))
        def _():
            wait(4)

        for j in range(4):
            o = 4 * (q - low) + j
            vector = all0[o].astype(F32)
            for b in range(held):
                row = jnp.concatenate([vector[b * blocks + c:b * blocks + c + 1] for c in range(blocks)], axis=1)
                total = total + nn(spread(row), turned_ref[held * o + b])
        return total

    ascent = lax.fori_loop(0, cubes - 2 * low, start_sum, jnp.zeros((ROWS, feats), F32))[0:1, :]
    scale = column_sq / samples + 1e-06
    stepped = w_start + ascent / (samples * scale)
    thresh = 1.0 / (4.0 * features * scale)
    primal = stepped - jnp.clip(stepped, -thresh, thresh)
    margin_scatter(primal, part1, got1, 1)
    merge_b(cubes - 2)
    merge_c(0)

    loop(1, cubes - 2, merge_c)
    merge_b(cubes - 1)
    merge_c(cubes - 2)
    loop(0, cubes - 1, merge_x)
    orders, places = [], []
    for b in range(blocks):
        order = (lax.broadcasted_iota(jnp.int32, (block, block), 0) == visit_ref[b:b + 1, :]).astype(F32)
        orders.append(order)
        places.append(order.T.astype(BF16))

    orders_half = [order.astype(BF16) for order in orders]
    twice = [jnp.concatenate([place, place], axis=1) for place in places]

    def upright(row, b):
        piece = row[:, b * block:(b + 1) * block]
        high = piece.astype(BF16).astype(F32)
        both = jnp.broadcast_to(jnp.concatenate([high, piece - high], axis=1), (block, 2 * block))
        return nt(twice[b], both.astype(BF16))

    alpha_zero = bound * frac_ref[...]
    for b in range(blocks):
        sign_c[b] = upright(sign, b)
        bound_c[b] = upright(bound, b)
        alpha_c[b] = upright(alpha_zero, b)
    pick_row = lax.broadcasted_iota(jnp.int32, (block, 2 * block), 0) % GROUP
    pick_lane = lax.broadcasted_iota(jnp.int32, (block, 2 * block), 1) // block
    for r in range(GROUP // 2):
        picks[r] = (pick_row == pick_lane + 2 * r).astype(F32).astype(BF16)

    total_wait(got1, 1).wait_recv()
    total_wait(got_d, 6).wait_recv()
    margin1, diag = jnp.sum(got1[...], axis=0), jnp.sum(got_d[...], axis=0)
    loss = jnp.sum(bound * jnp.square(jnp.maximum(0.0, 1.0 - sign * margin1)), axis=1, keepdims=True)
    penalty = jnp.sum(jnp.abs(primal), axis=1, keepdims=True)
    objective_part = loss / (2.0 * samples) + penalty / (4.0 * features)
    inverse = 0.5 / (diag + 1e-06)
    for b in range(blocks):
        inverse_c[b] = upright(inverse, b)
        margin_c[b] = upright(margin1, b)

    stage_wait(in_c, cube, 1, cube, send_c, recv_c).wait_recv()
    for half in range(2):
        gram_in[cube, half] = merged_c(cubes - 1, half)

    wait_d(0).wait_recv()
    packed = jnp.sum(gram_in[:, 0].astype(F32), axis=0)
    above, below = jnp.where(upper, packed, 0.0), jnp.where(lower, packed, 0.0)
    gap = row_at // GROUP - lane_at // GROUP

    def visited(a, b, piece):
        piece = nn(piece.astype(BF16), orders_half[b]).astype(BF16)
        return nn(places[a], piece)

    for b, piece in enumerate((above + above.T, below + below.T)):
        whole = visited(b, b, piece)
        square[b] = whole
        lagged = [jnp.where(gap == lag, whole, 0.0)[lag * GROUP:] for lag in (1, 2)]
        lagged = jnp.concatenate(lagged, axis=0).astype(BF16)
        for r in range(GROUP // 2):
            spots = nn(lagged, picks[r])
            for c in range(2):
                half = spots[:, c * block:(c + 1) * block]
                table[0, b, 2 * r + c, GROUP:, :] = half[:block - GROUP]
                table[1, b, 2 * r + c, 2 * GROUP:, :] = half[block - GROUP:]
    sub = lax.broadcasted_iota(jnp.int32, (GROUP, block), 0)
    lane = lax.broadcasted_iota(jnp.int32, (GROUP, block), 1)

    def fold(x):
        return x[0:8] + x[8:16]

    def total_of(terms):
        while len(terms) > 1:
            terms = [sum(terms[i:i + 2]) for i in range(0, len(terms), 2)]
        return terms[0]

    def sweep_block(b, offset):
        sets = block // GROUP
        seen, moved, pushes = jnp.zeros((8, block), F32), jnp.zeros((8, block), F32), []
        extra = [[] for _ in range(sets)]
        for s in range(sets):
            at = slice(s * GROUP, (s + 1) * GROUP)
            m = margin_c[b, at]
            if offset is not None:
                m = m + offset[at]
            for term in extra[s]:
                m = m + term
            now, side = alpha_c[b, at], sign_c[b, at]
            fresh = jnp.clip(now + (1.0 - side * m) * inverse_c[b, at], 0.0, bound_c[b, at])
            change = side * (fresh - now)
            alpha_c[b, at] = fresh
            moved = moved + fold(jnp.where(lane == sub + s * GROUP, change, 0.0))
            push = 2.0 * change
            pushes.append(push)
            steps = [jnp.broadcast_to(push[r:r + 1], (GROUP, block)) for r in range(GROUP)]
            if s + 3 < sets:
                seen = seen + fold(push * square[b, at])
                row = jnp.sum(seen, axis=0, keepdims=True)
                spot = jnp.where(lane == sub + (s + 3) * GROUP, row, 0.0)
                extra[s + 3].append(jnp.sum(spot, axis=1, keepdims=True))
            for lag in (2, 1):
                if s + lag < sets:
                    there = slice((s + lag) * GROUP, (s + lag + 1) * GROUP)
                    extra[s + lag].append(
                        total_of([steps[r] * table[lag - 1, b, r, there] for r in range(GROUP)])
                    )
        line = jnp.sum(moved, axis=0, keepdims=True)
        return nt(spread(line), orders_half[b])[0:1, :], pushes

    def passed_on(pushes):
        terms = [fold(push * between_c[s * GROUP:(s + 1) * GROUP]) for s, push in enumerate(pushes)]
        row = jnp.sum(total_of(terms), axis=0, keepdims=True)
        return jnp.sum(jnp.where(even, row, 0.0), axis=1, keepdims=True)

    first, pushes = sweep_block(0, None)
    wait_d(1).wait_recv()
    between_c[...] = visited(0, 1, jnp.sum(gram_in[:, 1].astype(F32), axis=0))
    second, _ = sweep_block(1, passed_on(pushes))
    own1[...] = jnp.concatenate([first, second], axis=0).astype(BF16)
    own_o[...] = jnp.broadcast_to(objective_part, (1, block))
    all_o[me] = own_o[...]
    gather_start(own1, all1, 1 + 3)
    peers(lambda peer: remote(own_o, all_o.at[me], send_sem.at[7], recv_sem.at[4], peer).start())
    update_one = back(all1, 4) * (2.0 / devices)
    margin_scatter(update_one, part2, got2, 2)
    total_wait(all_o, 7).wait_recv()
    out_ref[:, feats + rows:] = jnp.sum(all_o[...], axis=0)
    total_wait(got2, 2).wait_recv()
    margin2 = margin1 + jnp.sum(got2[...], axis=0)
    for b in range(blocks):
        margin_c[b] = upright(margin2, b)
    first, pushes = sweep_block(0, None)
    second, _ = sweep_block(1, passed_on(pushes))
    own2[...] = jnp.concatenate([first, second], axis=0).astype(BF16)
    gather_start(own2, all2, 2 + 3)
    def alpha_out():
        for b in range(blocks):
            spot = jnp.broadcast_to(jnp.sum(jnp.where(even, alpha_c[b], 0.0), axis=0, keepdims=True), (8, block))
            out_ref[:, feats + b * block:feats + (b + 1) * block] = nt(spot, orders[b], HIGH)[0:1, :]

    out_ref[:, :feats] = primal + update_one + back(all2, 5, alpha_out) * (2.0 / devices)

    for phase, ref in ((1, got1), (2, got2), (4, all1), (5, all2), (6, got_d), (7, all_o)):
        total_wait(ref, phase).wait_send()

    @pl.when(is_owner)
    def _():
        waiting(part0, owners - 1, send_sem.at[0], recv_sem.at[0]).wait_send()
        def sent(_):
            remote(own0, all0.at[0], send_sem.at[3], recv_sem.at[0], partner).wait_send()

        loop(0, devices - 1, sent)

    @pl.when(jnp.logical_not(is_owner))
    def _():
        waiting(part0, owners, send_sem.at[0], recv_sem.at[0]).wait_send()

    view = gram_in.at[pl.ds(0, cubes - 1)]
    remote(view, view, gram_send.at[0], gram_recv.at[0], partner).wait_send()

    stage_wait(in_a, 0, 4 * cubes, 0, send_a, recv_a).wait_send()
    stage_wait(in_b, 0, 2 * cubes, 0, send_b, recv_b).wait_send()
    stage_wait(in_c, 0, cubes, 0, send_c, recv_c).wait_send()


def split(packed, weights, alpha, objective):
    feats, rows = weights.shape[1], alpha.shape[1]
    weights[...] = packed[:, :feats]
    alpha[...] = packed[:, feats:feats + rows]
    objective[...] = packed[:, feats + rows:feats + rows + 1]


def body(devices, data_t, labels, sample_weight, w_start, alpha_start, visit_order):
    feats = data_t.shape[0]
    rows = alpha_start.shape[0]
    blocks, block = visit_order.shape
    cubes = devices // 8
    owners = cubes // 2 * 4
    span = (devices // owners * blocks, block)
    tiles = [x.reshape(owners, *span) for x in (labels, sample_weight)]
    labels = labels.reshape(devices, 1, rows)
    bound = sample_weight.reshape(devices, 1, rows)

    def grams(count):
        return pltpu.VMEM((count, rows // block, block, block), BF16)

    def semaphores(count):
        return pltpu.SemaphoreType.DMA((count,))

    def vectors(height, length):
        return pltpu.VMEM((devices, height, length), F32)

    vmem = pl.BlockSpec(memory_space=pltpu.VMEM)
    out = pl.pallas_call(
        functools.partial(kernel, devices),
        name="svm_rounds",
        out_shape=jax.ShapeDtypeStruct((1, feats + rows + block), F32),
        in_specs=[pl.BlockSpec(memory_space=pltpu.HBM)] * 8,
        out_specs=vmem,
        scratch_shapes=[
            pltpu.VMEM((owners, *span), F32), vectors(1, rows), vectors(1, rows), vectors(1, rows),
            pltpu.VMEM((devices, *span), F32), vectors(1, rows), vectors(1, rows), vectors(1, rows),
            pltpu.VMEM(span, BF16), pltpu.VMEM((blocks, block), BF16), pltpu.VMEM((blocks, block), BF16),
            pltpu.VMEM((1, block), F32), pltpu.VMEM((owners, *span), BF16),
            *[pltpu.VMEM((devices, blocks, block), BF16)] * 2, vectors(1, block),
            pltpu.VMEM(data_t.shape, BF16), pltpu.VMEM((devices, rows, feats), BF16), pltpu.VMEM((1, rows), jnp.int32), pltpu.VMEM((1, rows), F32),
            pltpu.VMEM(span, jnp.int32), pltpu.VMEM(span, F32),
            pltpu.VMEM((1, feats), F32), pltpu.VMEM((1, rows), F32), pltpu.VMEM((blocks, block), jnp.int32),
            pltpu.VMEM((feats, block), F32), grams(devices), grams(4 * cubes), grams(2 * cubes), grams(cubes),
            grams(4 * cubes), grams(2 * cubes), grams(cubes), grams(cubes),
            pltpu.VMEM((GROUP // 2, block, 2 * block), BF16), pltpu.VMEM((2, blocks, GROUP, block, block), F32),
            pltpu.VMEM((block, block), F32), *[pltpu.VMEM((blocks, block, block), F32)] * 6,
            semaphores(cubes), semaphores(7), semaphores(8), semaphores(5), semaphores(3 * cubes - 2 * (cubes // 4)),
            semaphores(1), semaphores(cubes), semaphores(1), semaphores(cubes), semaphores(1), semaphores(cubes),
            semaphores(1), semaphores(2),
        ],
        compiler_params=pltpu.CompilerParams(
            collective_id=0, has_side_effects=True, vmem_limit_bytes=48 * 1024 * 1024
        ),
    )(*[
        pltpu.with_memory_space_constraint(x, pltpu.HBM)
        for x in (data_t, labels, bound, *tiles, w_start[None], alpha_start[None], visit_order)
    ])
    weights, alpha, objective = pl.pallas_call(
        split,
        name="split",
        out_shape=(
            jax.ShapeDtypeStruct((1, feats), F32), jax.ShapeDtypeStruct((1, rows), F32), jax.ShapeDtypeStruct((1, 1), F32)
        ),
        in_specs=[vmem],
        out_specs=(vmem, vmem, vmem),
        compiler_params=pltpu.CompilerParams(vmem_limit_bytes=1024 * 1024),
    )(out)
    return weights[0], alpha[0], objective[0, 0]


def solution(mesh):
    placed = (P("shard", None), P(), P(), P("shard"), P("shard"), P("shard", None))
    return jax.shard_map(
        functools.partial(body, mesh.shape["shard"]), mesh=mesh, in_specs=placed,
        out_specs=(P("shard"), P("shard"), P()), check_vma=False,
    )
```
